128 devices in a mesh: cp: 128 (over x, y, z, core).
Axes of the slice: x: 4, y: 4, z: 4, core: 2. Of those that a mesh axis runs over, the one named last changes fastest.
Arguments:
- raw_inputs: bfloat16 [3584, 229376], P(None, 'cp'), may hold values from -6 to 6
- state_maps: bfloat16 [128, 229376], P(None, 'cp'), may hold values from -6 to 6
- step_size: float32 [56, 229376], P(None, 'cp'), may hold values from 0 to 1, as said below
- log_decay: float32 [56, 229376], P(None, 'cp'), may hold values from -2 to 0, as said below
- conv_weight: float32 [4, 3584], replicated, may hold values from -3 to 3
- conv_bias: float32 [3584], replicated, may hold values from -3 to 3
- skip_gain: float32 [56], replicated, may hold values from 0.5 to 1.5
Outputs:
- layer_output: bfloat16 [3584, 229376], P(None, 'cp')
The draws below stay inside these ranges and needn't reach their ends.
Inputs may be any that keep to these rules, and one draw needn't show every extreme that they name: step_size is positive. log_decay is never positive.
All inputs are finite; a program needn't handle non-finite values.
Results may differ from the reference program's by a relative error of at most 0.0058.
Values may be sent and summed in bfloat16 or wider, within the bound.
No kernel may reach another device: no remote copies, remote signals or barrier semaphores. Data moves between devices by JAX's collectives and lax.ppermute only.
A program may use at most 192 MiB of HBM per device.

```python
import jax
import jax.numpy as jnp
from jax import lax

HEADS = 56
HEAD_DIM = 64
STATE = 64
BLOCK = 256
CONVOLUTION_TAPS = 4
TOK_DEV = 1792
TOKENS = 229376


def decay_and_step(key):
    folded = jax.random.fold_in(key, 41)
    subkeys = jax.random.split(folded, 7)
    ranking = jax.random.permutation(subkeys[0], HEADS)
    slow_heads = ranking < HEADS // 2
    chain_total = jnp.exp(jax.random.uniform(subkeys[1], (HEADS,), jnp.float32, jnp.log(0.3), jnp.log(0.9)))
    slow_rate = chain_total / (1.0 * TOKENS)
    fast_rate = jnp.exp(jax.random.uniform(subkeys[2], (HEADS,), jnp.float32, jnp.log(1.0 / 50.0), jnp.log(1.0 / 30.0)))
    decay_rate = jnp.where(slow_heads, slow_rate, fast_rate)
    head_step = jnp.where(slow_heads, 0.2 / jnp.sqrt(1.0 * TOKENS), 0.2 * jnp.sqrt(2.0 * fast_rate))
    blocks = TOKENS // TOK_DEV
    device_factor = jnp.exp(jax.random.uniform(subkeys[3], (HEADS, blocks), jnp.float32, -0.5, 0.5))
    device_factor = jnp.repeat(device_factor, TOK_DEV, axis=1)
    token_factor = jax.random.uniform(subkeys[4], (HEADS, TOKENS), jnp.float32, 0.5, 1.5)
    logarithmic_decay = -(decay_rate[:, None] * device_factor * token_factor)
    device_positions = jax.random.randint(subkeys[5], (3, HEADS), 0, TOKENS)
    training_losses = jax.random.uniform(subkeys[6], (3, HEADS), jnp.float32, 0.22, 0.43)
    token_position = lax.broadcasted_iota(jnp.int32, (HEADS, TOKENS), 1)
    for segment_index in range(3):
        logarithmic_decay = logarithmic_decay - jnp.where(token_position == device_positions[segment_index][:, None], training_losses[segment_index][:, None], 0.0)
    step_sizes = head_step[:, None] * token_factor
    return (logarithmic_decay, step_sizes)


def draw_step_size(key, part):
    return decay_and_step(key)[1].astype(jnp.float32)


def draw_log_decay(key, part):
    return decay_and_step(key)[0].astype(jnp.float32)


def shard_levels(stream_key, dims, shards, least, top_value):
    loudness, own = 1.0, jax.random.fold_in(stream_key, 6)
    for axis_at, parts in shards:
        heights = jnp.exp(jax.random.uniform(jax.random.fold_in(own, axis_at), (parts,), jnp.float32, least / len(shards), top_value / len(shards)))
        loudness = loudness * jnp.repeat(heights, dims[axis_at] // parts).reshape([-1 if axis == axis_at else 1 for axis in range(len(dims))])
    return loudness


def noise(stream_key, extent, deviation, reach, cuts=(), held_as=jnp.bfloat16):
    factor_of = shard_levels(stream_key, extent, cuts, -0.22, 0.18) if cuts else 1.0
    array = jax.random.normal(stream_key, extent, jnp.float32) * deviation * factor_of
    return jnp.minimum(jnp.maximum(array, -reach), reach).astype(held_as)


def setup_inputs(seed: int = 0) -> dict:
    key_of = jax.random.split(jax.random.key(seed), 8)
    return {
        "raw_inputs": noise(key_of[0], (HEADS * HEAD_DIM, TOKENS), 1.0, 6.0, ((1, 128),)),
        "state_maps": noise(key_of[1], (2 * STATE, TOKENS), 1.0, 6.0, ((1, 128),)),
        "step_size": draw_step_size(jax.random.fold_in(key_of[7], 71), 0),
        "log_decay": draw_log_decay(jax.random.fold_in(key_of[7], 71), 0),
        "conv_weight": noise(key_of[4], (CONVOLUTION_TAPS, HEADS * HEAD_DIM), CONVOLUTION_TAPS ** -0.5, 3.0, (), jnp.float32),
        "conv_bias": noise(key_of[5], (HEADS * HEAD_DIM,), 0.5, 3.0, (), jnp.float32),
        "skip_gain": jnp.clip(jax.random.uniform(key_of[6], (HEADS,), jnp.float32, 0.5, 1.5), 0.5, 1.5),
    }


def reference(raw_inputs, state_maps, step_size, log_decay, conv_weight, conv_bias, skip_gain):
    conv_taps = conv_weight.shape[0]
    block_count = TOKENS // BLOCK
    channels = HEADS * HEAD_DIM
    raw_blocks = raw_inputs.T.reshape(block_count, BLOCK, channels)
    map_blocks = state_maps.T.reshape(block_count, BLOCK, 2 * STATE)
    step_blocks = jnp.transpose(step_size.reshape(HEADS, block_count, BLOCK), (1, 0, 2))
    decay_blocks = jnp.transpose(log_decay.reshape(HEADS, block_count, BLOCK), (1, 0, 2))
    causal = jnp.arange(BLOCK)[:, None] >= jnp.arange(BLOCK)[None, :]

    def advance(carry_in, pieces):
        state_now, prior_rows = carry_in
        block_raw, block_transforms, block_steps, block_decay = pieces
        extended = jnp.concatenate([prior_rows, block_raw], axis=0).astype(jnp.float32)
        convolved = jnp.zeros((BLOCK, channels), jnp.float32) + conv_bias[None, :]
        for offset in range(conv_taps):
            convolved = convolved + conv_weight[offset][None, :] * extended[offset:offset + BLOCK]
        values = jax.nn.silu(convolved).astype(jnp.bfloat16)
        inputs = values.reshape(BLOCK, HEADS, HEAD_DIM).astype(jnp.float32)
        key_rows = block_transforms[:, :STATE]
        query_rows = block_transforms[:, STATE:]
        sums = jnp.cumsum(block_decay, axis=1)
        affinity = jnp.dot(query_rows, key_rows.T, preferred_element_type=jnp.float32)
        decay_gaps = jnp.where(causal[None], sums[:, :, None] - sums[:, None, :], 0.0)
        weights = jnp.where(causal[None], affinity[None] * jnp.exp(decay_gaps) * block_steps[:, None, :], 0.0).astype(jnp.bfloat16)
        local_out = jnp.einsum("hij,jhp->ihp", weights.astype(jnp.float32), inputs)
        entering_b = state_now.astype(jnp.bfloat16).astype(jnp.float32)
        carried = jnp.einsum("in,hnp->ihp", query_rows.astype(jnp.float32), entering_b) * jnp.exp(sums).T[:, :, None]
        result_rows = local_out + carried + skip_gain[None, :, None] * inputs
        block_end = sums[:, BLOCK - 1:]
        scaled = (key_rows.astype(jnp.float32)[None] * (jnp.exp(block_end - sums) * block_steps)[:, :, None]).astype(jnp.bfloat16)
        block_state = jnp.einsum("hjn,jhp->hnp", scaled.astype(jnp.float32), inputs)
        next_state = jnp.exp(block_end)[:, :, None] * state_now + block_state
        next_rows = block_raw[BLOCK - (conv_taps - 1):]
        return (next_state, next_rows), result_rows.reshape(BLOCK, channels).astype(jnp.bfloat16)

    start_state = jnp.zeros((HEADS, STATE, HEAD_DIM), jnp.float32)
    start_rows = jnp.zeros((conv_taps - 1, channels), jnp.bfloat16)
    final_carry, outputs = lax.scan(advance, (start_state, start_rows), (raw_blocks, map_blocks, step_blocks, decay_blocks))
    return outputs.reshape(TOKENS, channels).T
```

```python
import functools

import jax
import jax.numpy as jnp
from jax import lax
from jax.experimental import pallas as pl
from jax.experimental.pallas import tpu as pltpu
from jax.sharding import PartitionSpec as P

CHUNK = 128
GROUP = 8
HEAD_DIM = 64
STATE = 64
ROWS = GROUP * HEAD_DIM
LOG2E = 1.4426950408889634
F32 = jnp.float32
BF16 = jnp.bfloat16


def dot_nt(a, b):
    return lax.dot_general(a, b, (((1,), (1,)), ((), ())), preferred_element_type=F32)


def chunk_sums(log_decay, chunks):
    stacked = jnp.concatenate(
        [log_decay[:, c * CHUNK : (c + 1) * CHUNK] for c in range(chunks)], axis=0
    ) * LOG2E
    row = lax.broadcasted_iota(jnp.int32, (CHUNK, CHUNK), 0)
    col = lax.broadcasted_iota(jnp.int32, (CHUNK, CHUNK), 1)
    upper = jnp.where(row <= col, 1.0, 0.0).astype(F32)
    summed = lax.dot_general(
        stacked, upper, (((1,), (0,)), ((), ())),
        precision=lax.Precision.HIGHEST, preferred_element_type=F32,
    )
    return [summed[c * GROUP : (c + 1) * GROUP] for c in range(chunks)]


def values_kernel(chunks, raw_ref, halo_ref, maps_ref, step_ref, decay_ref, taps_ref, bias_ref,
                  x_ref, sums_ref, lead_ref, msg_ref, taps_scr, d_scr, xd_scr, part_scr):
    g = pl.program_id(0)
    half_lanes = 4 * HEAD_DIM
    sums = chunk_sums(decay_ref[...], chunks)
    ends = [jnp.broadcast_to(s[:, CHUNK - 1 :], (GROUP, CHUNK)) for s in sums]
    before = jnp.zeros((GROUP, CHUNK), F32)
    for c in range(chunks):
        at = slice(c * CHUNK, (c + 1) * CHUNK)
        sums_ref[:, at] = sums[c]
        lead_ref[:, at] = jnp.exp2(before + sums[c])
        before = before + ends[c]
    after = jnp.zeros((GROUP, CHUNK), F32)
    for c in reversed(range(chunks)):
        at = slice(c * CHUNK, (c + 1) * CHUNK)
        to_end = jnp.exp2((ends[c] - sums[c]) + after) * step_ref[:, at]
        for h in range(GROUP):
            d_scr[h, :, at] = jnp.broadcast_to(to_end[h : h + 1, :], (8, CHUNK))
        after = after + ends[c]
    total = jnp.exp2(before)

    lane8 = lax.broadcasted_iota(jnp.int32, (GROUP, CHUNK), 1)
    sub8 = lax.broadcasted_iota(jnp.int32, (GROUP, CHUNK), 0)
    own = lane8 == g * 4 + lax.rem(sub8, 4)
    placed = jnp.where(own, total, 0.0)

    @pl.when(g == 0)
    def _():
        part_scr[...] = jnp.zeros_like(part_scr)

    part_scr[...] += placed

    taps = jnp.concatenate([taps_ref[...], bias_ref[...], jnp.zeros((3, ROWS), F32)], axis=0) * 0.5
    taps_scr[...] = jnp.transpose(taps)

    lane = lax.broadcasted_iota(jnp.int32, (16, CHUNK), 1)
    inside = [lane >= k for k in range(4)]
    keys = maps_ref[:STATE, :]

    def pair_body(pair, carry):
        for r in range(8):
            rows = pl.ds(pl.multiple_of(pair * 128 + r * 16, 16), 16)
            local = slice(r * 16, (r + 1) * 16)
            cols = taps_scr[rows, :]
            w = [jnp.broadcast_to(cols[:, k : k + 1], (16, CHUNK)) for k in range(5)]
            head = pair * 2 + r // 4
            last = halo_ref[rows, :].astype(F32)
            prior = [None] + [pltpu.roll(last, k, 1) for k in (1, 2, 3)]
            for c in range(chunks):
                at = slice(c * CHUNK, (c + 1) * CHUNK)
                now = raw_ref[rows, at].astype(F32)
                rolled = [None] + [pltpu.roll(now, k, 1) for k in (1, 2, 3)]
                h = w[4] + w[3] * now
                for k in (1, 2, 3):
                    h = h + w[3 - k] * jnp.where(inside[k], rolled[k], prior[k])
                prior = rolled
                value = h + h * jnp.tanh(h)
                x_ref[rows, at] = value.astype(BF16)
                to_end = d_scr[head, :, at]
                to_end = jnp.concatenate([to_end, to_end], axis=0)
                xd_scr[local, at] = (value * to_end).astype(BF16)
        state = dot_nt(keys, xd_scr[...])
        lanes = pl.ds(pl.multiple_of(g * half_lanes + lax.rem(pair, 2) * 128, 128), 128)
        msg_ref[lax.div(pair, 2), :, lanes] = state.astype(BF16)
        return carry

    lax.fori_loop(0, 4, pair_body, 0)

    @pl.when(g == pl.num_programs(0) - 1)
    def _():
        acc = part_scr[...]
        lane1 = lax.broadcasted_iota(jnp.int32, (1, CHUNK), 1)
        for s in range(2):
            d = acc[4 * s : 4 * s + 1] + acc[4 * s + 1 : 4 * s + 2]
            d = d + (acc[4 * s + 2 : 4 * s + 3] + acc[4 * s + 3 : 4 * s + 4])
            hi = d.astype(BF16).astype(F32)
            mid = (d - hi).astype(BF16).astype(F32)
            low = (d - hi) - mid
            row = hi + pltpu.roll(jnp.broadcast_to(mid, (8, CHUNK)), 32, 1)[:1]
            row = row + pltpu.roll(jnp.broadcast_to(low, (8, CHUNK)), 64, 1)[:1]
            base = msg_ref.shape[2] - CHUNK
            msg_ref[s, :, base:] = jnp.broadcast_to(row, (STATE, CHUNK)).astype(BF16)


def scan_kernel(got_ref, out_ref):
    count = got_ref.shape[0]
    width = out_ref.shape[1]
    row = lax.broadcasted_iota(jnp.int32, (count, 128), 0)
    part = lax.broadcasted_iota(jnp.int32, (128, 128), 0)
    lane = lax.broadcasted_iota(jnp.int32, (128, 128), 1)
    parts = got_ref[:, width:]
    for t in range(width // 128):
        at = slice(t * 128, (t + 1) * 128)
        head = t * 2 + lax.div(lane, 64)
        pick = jnp.where((lax.rem(part, 32) == head) & (part < 96), 1.0, 0.0).astype(BF16)
        decay = jnp.dot(parts, pick, preferred_element_type=F32)
        total = got_ref[:, at].astype(F32)
        step = 1
        while step < count:
            keep = row >= step
            total = total + decay * jnp.where(keep, pltpu.roll(total, step, 0), 0.0)
            decay = decay * jnp.where(keep, pltpu.roll(decay, step, 0), 1.0)
            step *= 2
        out_ref[:, at] = jnp.where(row >= 1, pltpu.roll(total, 1, 0), 0.0).astype(BF16)


def local_kernel(chunks, *refs):
    x_ref, maps_ref, step_ref, sums_ref, skip_ref = refs[:5]
    y_ref, state_scr = refs[-2:]
    state_scr[...] = jnp.zeros_like(state_scr)
    jdx = lax.broadcasted_iota(jnp.int32, (CHUNK, CHUNK), 0)
    idx = lax.broadcasted_iota(jnp.int32, (CHUNK, CHUNK), 1)
    causal = idx >= jdx

    def chunk_body(c, carry):
        at = pl.ds(pl.multiple_of(c * CHUNK, CHUNK), CHUNK)
        keys = maps_ref[:STATE, at]
        queries = maps_ref[STATE:, at]
        affinity = jnp.dot(jnp.transpose(keys), queries, preferred_element_type=F32)
        affinity = jnp.where(causal, affinity, 0.0)
        queries32 = queries.astype(F32)
        sums = sums_ref[:, at]
        steps = step_ref[:, at]
        ends = jnp.broadcast_to(sums[:, CHUNK - 1 :], (GROUP, CHUNK))
        rise = jnp.exp2(sums)
        fall = jnp.exp2(ends - sums) * steps
        columns = jnp.transpose(jnp.log2(steps) - sums)
        scaled = []
        for h in range(GROUP):
            rows = slice(h * HEAD_DIM, (h + 1) * HEAD_DIM)
            x = x_ref[rows, at]
            x32 = x.astype(F32)
            gaps = sums[h : h + 1, :] + columns[:, h : h + 1]
            weights = (affinity * jnp.exp2(jnp.minimum(gaps, 0.0))).astype(BF16)
            risen = (queries32 * rise[h : h + 1, :]).astype(BF16)
            state = state_scr[rows, :]
            left = jnp.concatenate([x, state.astype(BF16)], axis=1)
            right = jnp.concatenate([weights, risen], axis=0)
            out = jnp.dot(left, right, preferred_element_type=F32)
            out = out + x32 * skip_ref[rows, :1]
            y_ref[rows, at] = out.astype(BF16)
            scaled.append((x32 * fall[h : h + 1, :]).astype(BF16))
        update = dot_nt(jnp.concatenate(scaled, axis=0), keys)
        for h in range(GROUP):
            rows = slice(h * HEAD_DIM, (h + 1) * HEAD_DIM)
            decay = jnp.broadcast_to(rise[h : h + 1, CHUNK - 1 :], (HEAD_DIM, STATE))
            state_scr[rows, :] = state_scr[rows, :] * decay + update[rows]
        return carry

    lax.fori_loop(0, chunks, chunk_body, 0)


def carried_kernel(chunks, y_ref, maps_ref, lead_ref, enter_ref, out_ref):
    first = jnp.transpose(enter_ref[0])
    second = jnp.transpose(enter_ref[1])
    entering = jnp.concatenate([first, second], axis=0)
    for c in range(chunks // 2):
        at = slice(c * 256, (c + 1) * 256)
        carried = jnp.dot(entering, maps_ref[STATE:, at], preferred_element_type=F32)
        for h in range(GROUP):
            rows = slice(h * HEAD_DIM, (h + 1) * HEAD_DIM)
            add = carried[rows] * lead_ref[h : h + 1, at]
            out_ref[rows, at] = (y_ref[rows, at].astype(F32) + add).astype(BF16)


def local(raw_inputs, state_maps, step_size, log_decay, conv_weight, conv_bias, skip_gain, axis):
    channels, tokens = raw_inputs.shape
    heads = skip_gain.shape[0]
    groups = heads // GROUP
    chunks = tokens // CHUNK
    count = lax.axis_size(axis)
    half = channels // 2

    tail = lax.ppermute(
        raw_inputs[:, tokens - 3 :], axis, [(i, i + 1) for i in range(count - 1)]
    )
    halo = jnp.pad(tail, ((0, 0), (CHUNK - 3, 0)))

    block = lambda g: (g, 0)
    whole = lambda g: (0, 0)
    big = pl.BlockSpec((ROWS, tokens), block)
    rows8 = pl.BlockSpec((GROUP, tokens), block)
    maps = pl.BlockSpec((2 * STATE, tokens), whole)
    cost = lambda us: pl.CostEstimate(
        flops=int(us * 5e8), bytes_accessed=int(us * 1e6), transcendentals=0
    )
    params = pltpu.CompilerParams(dimension_semantics=("arbitrary",))

    values, sums, lead, message = pl.pallas_call(
        functools.partial(values_kernel, chunks),
        grid=(groups,),
        in_specs=[
            big,
            pl.BlockSpec((ROWS, CHUNK), block),
            maps,
            rows8,
            rows8,
            pl.BlockSpec((4, ROWS), lambda g: (0, g)),
            pl.BlockSpec((1, ROWS), lambda g: (0, g)),
        ],
        out_specs=[big, rows8, rows8, pl.BlockSpec((2, STATE, half + CHUNK), lambda g: (0, 0, 0))],
        out_shape=[
            jax.ShapeDtypeStruct((channels, tokens), BF16),
            jax.ShapeDtypeStruct((heads, tokens), F32),
            jax.ShapeDtypeStruct((heads, tokens), F32),
            jax.ShapeDtypeStruct((2, STATE, half + CHUNK), BF16),
        ],
        scratch_shapes=[
            pltpu.VMEM((ROWS, 8), F32),
            pltpu.VMEM((GROUP, 8, tokens), F32),
            pltpu.VMEM((128, tokens), BF16),
            pltpu.VMEM((GROUP, CHUNK), F32),
        ],
        compiler_params=params,
        cost_estimate=cost(20),
        name="values",
    )(raw_inputs, halo, state_maps, step_size, log_decay, conv_weight, conv_bias.reshape(1, channels))

    got = lax.all_to_all(message.reshape(2 * STATE, half + CHUNK), axis, 0, 0, tiled=True)

    skip = jnp.broadcast_to(jnp.repeat(skip_gain, HEAD_DIM)[:, None], (channels, 128))

    def local_part(first, number, previous):
        shift = lambda g: (g + first, 0)
        specs = [
            pl.BlockSpec((ROWS, tokens), shift),
            maps,
            pl.BlockSpec((GROUP, tokens), shift),
            pl.BlockSpec((GROUP, tokens), shift),
            pl.BlockSpec((ROWS, 128), shift),
        ]
        arrays = [values, state_maps, step_size, sums, skip]
        alias = {}
        if previous is not None:
            specs.append(pl.BlockSpec(memory_space=pl.ANY))
            arrays.append(previous)
            alias = {5: 0}
        return pl.pallas_call(
            functools.partial(local_kernel, chunks),
            grid=(number,),
            in_specs=specs,
            out_specs=pl.BlockSpec((ROWS, tokens), shift),
            out_shape=jax.ShapeDtypeStruct((channels, tokens), BF16),
            scratch_shapes=[pltpu.VMEM((ROWS, STATE), F32)],
            input_output_aliases=alias,
            compiler_params=params,
            cost_estimate=cost(4 * number),
            name="inside",
        )(*arrays)

    early = groups // 2
    partial = local_part(0, early, None)

    entering = pl.pallas_call(
        scan_kernel,
        in_specs=[pl.BlockSpec(memory_space=pltpu.VMEM)],
        out_specs=pl.BlockSpec(memory_space=pltpu.VMEM),
        out_shape=jax.ShapeDtypeStruct((count, half), BF16),
        cost_estimate=cost(3),
        name="scan",
    )(got)
    back = lax.all_to_all(entering, axis, 0, 0, tiled=True).reshape(2, STATE, half)

    partial = local_part(early, groups - early, partial)

    return pl.pallas_call(
        functools.partial(carried_kernel, chunks),
        grid=(groups,),
        in_specs=[
            big,
            maps,
            rows8,
            pl.BlockSpec((2, STATE, 4 * HEAD_DIM), lambda g: (0, 0, g)),
        ],
        out_specs=big,
        out_shape=jax.ShapeDtypeStruct((channels, tokens), BF16),
        input_output_aliases={0: 0},
        compiler_params=params,
        cost_estimate=cost(8),
        name="carried",
    )(partial, state_maps, lead, back)


def solution(mesh):
    axis = mesh.axis_names[0]
    return jax.shard_map(
        functools.partial(local, axis=axis),
        mesh=mesh,
        in_specs=(P(None, axis),) * 4 + (P(),) * 3,
        out_specs=P(None, axis),
        check_vma=False,
    )
```

```python
import functools

import jax
import jax.numpy as jnp
from jax import lax
from jax.experimental import pallas as pl
from jax.experimental.pallas import tpu as pltpu
from jax.sharding import PartitionSpec as P

CHUNK = 128
SEGMENT = 16
GROUP = 8
HEAD_DIM = 64
STATE = 64
ROWS = GROUP * HEAD_DIM
LOG2E = 1.4426950408889634
F32 = jnp.float32
BF16 = jnp.bfloat16


def dot_nt(a, b):
    return lax.dot_general(a, b, (((1,), (1,)), ((), ())), preferred_element_type=F32)


def chunk_sums(log_decay, chunks):
    stacked = jnp.concatenate(
        [log_decay[:, c * CHUNK : (c + 1) * CHUNK] for c in range(chunks)], axis=0
    ) * LOG2E
    row = lax.broadcasted_iota(jnp.int32, (CHUNK, CHUNK), 0)
    col = lax.broadcasted_iota(jnp.int32, (CHUNK, CHUNK), 1)
    upper = jnp.where(row <= col, 1.0, 0.0).astype(F32)
    summed = lax.dot_general(
        stacked, upper, (((1,), (0,)), ((), ())),
        precision=lax.Precision.HIGHEST, preferred_element_type=F32,
    )
    return [summed[c * GROUP : (c + 1) * GROUP] for c in range(chunks)]


def values_kernel(chunks, raw_ref, halo_ref, maps_ref, step_ref, decay_ref, taps_ref, bias_ref,
                  x_ref, sums_ref, lead_ref, msg_ref, d_scr, xd_scr):
    sums = chunk_sums(decay_ref[...], chunks)
    ends = [jnp.broadcast_to(s[:, CHUNK - 1 :], (GROUP, CHUNK)) for s in sums]
    before = jnp.zeros((GROUP, CHUNK), F32)
    for c in range(chunks):
        at = slice(c * CHUNK, (c + 1) * CHUNK)
        sums_ref[:, at] = sums[c]
        lead_ref[:, at] = jnp.exp2(before + sums[c])
        before = before + ends[c]
    after = jnp.zeros((GROUP, CHUNK), F32)
    for c in reversed(range(chunks)):
        at = slice(c * CHUNK, (c + 1) * CHUNK)
        to_end = jnp.exp2((ends[c] - sums[c]) + after) * step_ref[:, at]
        for h in range(GROUP):
            d_scr[h, :, at] = jnp.broadcast_to(to_end[h : h + 1, :], (8, CHUNK))
        after = after + ends[c]
    total = jnp.exp2(before)
    hi = total.astype(BF16).astype(F32)
    low = total - hi
    for h in range(GROUP):
        tile = jnp.concatenate(
            [jnp.broadcast_to(hi[h : h + 1], (8, CHUNK)), jnp.broadcast_to(low[h : h + 1], (8, CHUNK))], axis=0
        ).astype(BF16)
        msg_ref[2 * h, 16:, :] = tile
        msg_ref[2 * h + 1, 16:, :] = tile

    keys = maps_ref[:STATE, :]
    row = lax.broadcasted_iota(jnp.int32, (HEAD_DIM, 4 * HEAD_DIM), 0)
    col = lax.broadcasted_iota(jnp.int32, (HEAD_DIM, 4 * HEAD_DIM), 1)
    diagonal = row == lax.rem(col, HEAD_DIM)
    lane = lax.broadcasted_iota(jnp.int32, (HEAD_DIM, CHUNK), 1)
    inside = [lane >= k for k in range(4)]

    def head_body(head, carry):
        rows = pl.ds(pl.multiple_of(head * HEAD_DIM, HEAD_DIM), HEAD_DIM)
        taps = jnp.broadcast_to(taps_ref[head, :1, :], (HEAD_DIM, 4 * HEAD_DIM))
        taps = jnp.where(diagonal, taps, 0.0)
        taps_hi = taps.astype(BF16)
        taps_low = (taps - taps_hi.astype(F32)).astype(BF16)
        left = jnp.concatenate([taps_hi, taps_low], axis=0)
        bias = jnp.broadcast_to(bias_ref[rows, :1], (HEAD_DIM, 2 * CHUNK))
        last = halo_ref[rows, :]
        prior = [None] + [pltpu.roll(last, k, 1) for k in (1, 2, 3)]
        for t in range(chunks // 2):
            columns = []
            for c in (2 * t, 2 * t + 1):
                now = raw_ref[rows, c * CHUNK : (c + 1) * CHUNK]
                rolled = [None] + [pltpu.roll(now, k, 1) for k in (1, 2, 3)]
                moved = [jnp.where(inside[k], rolled[k], prior[k]) for k in (3, 2, 1)]
                columns.append(jnp.concatenate(moved + [now], axis=0))
                prior = rolled
            at = slice(2 * t * CHUNK, 2 * (t + 1) * CHUNK)
            both = jnp.dot(left, jnp.concatenate(columns, axis=1), preferred_element_type=F32)
            half = (both[:HEAD_DIM] + both[HEAD_DIM:]) + bias
            value = half + half * jnp.tanh(half)
            x_ref[rows, at] = value.astype(BF16)
            to_end = d_scr[head, :, at]
            to_end = jnp.concatenate([to_end] * 8, axis=0)
            xd_scr[:, at] = (value * to_end).astype(BF16)
        state = dot_nt(xd_scr[...], keys).astype(BF16)
        for k in range(2):
            msg_ref[2 * head + k, :16, :] = jnp.concatenate(
                [state[32 * k : 32 * k + 16], state[32 * k + 16 : 32 * k + 32]], axis=1
            )
        return carry

    lax.fori_loop(0, GROUP, head_body, 0)


def scan_kernel(got_ref, out_ref):
    entering = jnp.zeros((16, 128), F32)
    for d in range(got_ref.shape[0]):
        out_ref[d] = entering.astype(BF16)
        parts = got_ref[d, 16:, :].astype(F32)
        decay = parts[:8] + parts[8:]
        decay = jnp.concatenate([decay, decay], axis=0)
        entering = decay * entering + got_ref[d, :16, :].astype(F32)


def local_kernel(chunks, *refs):
    x_ref, maps_ref, step_ref, sums_ref, skip_ref = refs[:5]
    y_ref, state_scr = refs[-2:]
    state_scr[...] = jnp.zeros_like(state_scr)
    jdx = lax.broadcasted_iota(jnp.int32, (CHUNK, CHUNK), 0)
    idx = lax.broadcasted_iota(jnp.int32, (CHUNK, CHUNK), 1)
    causal = idx >= jdx
    segment = lax.div(lax.broadcasted_iota(jnp.int32, (GROUP, CHUNK), 1), SEGMENT)

    def one_chunk(c):
        at = pl.ds(pl.multiple_of(c * CHUNK, CHUNK), CHUNK)
        keys = maps_ref[:STATE, at]
        queries = maps_ref[STATE:, at]
        affinity = jnp.dot(jnp.transpose(keys), queries, preferred_element_type=F32)
        affinity = jnp.where(causal, affinity, 0.0)
        queries32 = queries.astype(F32)
        sums = sums_ref[:, at]
        steps = step_ref[:, at]
        ends = jnp.broadcast_to(sums[:, CHUNK - 1 :], (GROUP, CHUNK))
        rise = jnp.exp2(sums)
        fall = jnp.exp2(ends - sums) * steps
        marks = ends
        grown = []
        for b in range(CHUNK // SEGMENT):
            last = (b + 1) * SEGMENT - 1
            mark = jnp.broadcast_to(sums[:, last : last + 1], (GROUP, CHUNK))
            grown.append(jnp.exp2(jnp.minimum(sums - mark, 100.0)))
            marks = jnp.where(segment == b, mark, marks)
        shrunk = jnp.exp2(marks - sums) * steps
        scaled = []
        for h in range(GROUP):
            rows = slice(h * HEAD_DIM, (h + 1) * HEAD_DIM)
            x = x_ref[rows, at]
            x32 = x.astype(F32)
            pieces = [
                affinity[b * SEGMENT : (b + 1) * SEGMENT] * grown[b][h : h + 1, :]
                for b in range(CHUNK // SEGMENT)
            ]
            weights = jnp.concatenate(pieces, axis=0).astype(BF16)
            risen = (queries32 * rise[h : h + 1, :]).astype(BF16)
            stepped = (x32 * shrunk[h : h + 1, :]).astype(BF16)
            state = state_scr[rows, :]
            left = jnp.concatenate([stepped, state.astype(BF16)], axis=1)
            right = jnp.concatenate([weights, risen], axis=0)
            out = jnp.dot(left, right, preferred_element_type=F32)
            out = out + x32 * skip_ref[rows, :1]
            y_ref[rows, at] = out.astype(BF16)
            scaled.append((x32 * fall[h : h + 1, :]).astype(BF16))
        update = dot_nt(jnp.concatenate(scaled, axis=0), keys)
        for h in range(GROUP):
            rows = slice(h * HEAD_DIM, (h + 1) * HEAD_DIM)
            decay = jnp.broadcast_to(rise[h : h + 1, CHUNK - 1 :], (HEAD_DIM, STATE))
            state_scr[rows, :] = state_scr[rows, :] * decay + update[rows]

    def body(t, carry):
        for k in range(2):
            one_chunk(2 * t + k)
        return carry

    lax.fori_loop(0, chunks // 2, body, 0)


def carried_kernel(chunks, y_ref, maps_ref, lead_ref, enter_ref, out_ref):
    for c in range(chunks // 2):
        at = slice(c * 256, (c + 1) * 256)
        queries = maps_ref[STATE:, at]
        pieces = []
        for h in range(2 * GROUP):
            tile = enter_ref[h]
            pieces += [tile[:, :STATE], tile[:, STATE:]]
        entering = jnp.concatenate(pieces, axis=0)
        carried = jnp.dot(entering, queries, preferred_element_type=F32)
        for h in range(GROUP):
            rows = slice(h * HEAD_DIM, (h + 1) * HEAD_DIM)
            add = carried[rows] * lead_ref[h : h + 1, at]
            out_ref[rows, at] = (y_ref[rows, at].astype(F32) + add).astype(BF16)


def local(raw_inputs, state_maps, step_size, log_decay, conv_weight, conv_bias, skip_gain, axis):
    channels, tokens = raw_inputs.shape
    heads = skip_gain.shape[0]
    groups = heads // GROUP
    chunks = tokens // CHUNK
    count = lax.axis_size(axis)

    tail = lax.ppermute(
        raw_inputs[:, tokens - 3 :], axis, [(i, i + 1) for i in range(count - 1)]
    )
    halo = jnp.pad(tail, ((0, 0), (CHUNK - 3, 0)))

    taps = 0.5 * jnp.transpose(conv_weight.reshape(4, heads, HEAD_DIM), (1, 0, 2))
    taps = taps.reshape(heads, 1, 4 * HEAD_DIM)
    bias = jnp.broadcast_to(0.5 * conv_bias[:, None], (channels, 128))

    block = lambda g: (g, 0)
    whole = lambda g: (0, 0)
    big = pl.BlockSpec((ROWS, tokens), block)
    rows8 = pl.BlockSpec((GROUP, tokens), block)
    maps = pl.BlockSpec((2 * STATE, tokens), whole)
    cost = lambda us: pl.CostEstimate(
        flops=int(us * 5e8), bytes_accessed=int(us * 1e6), transcendentals=0
    )
    params = pltpu.CompilerParams(dimension_semantics=("arbitrary",))

    values, sums, lead, message = pl.pallas_call(
        functools.partial(values_kernel, chunks),
        grid=(groups,),
        in_specs=[
            big,
            pl.BlockSpec((ROWS, CHUNK), block),
            maps,
            rows8,
            rows8,
            pl.BlockSpec((GROUP, 1, 4 * HEAD_DIM), lambda g: (g, 0, 0)),
            pl.BlockSpec((ROWS, 128), block),
        ],
        out_specs=[big, rows8, rows8, pl.BlockSpec((2 * GROUP, 32, 128), lambda g: (g, 0, 0))],
        out_shape=[
            jax.ShapeDtypeStruct((channels, tokens), BF16),
            jax.ShapeDtypeStruct((heads, tokens), F32),
            jax.ShapeDtypeStruct((heads, tokens), F32),
            jax.ShapeDtypeStruct((count, 32, 128), BF16),
        ],
        scratch_shapes=[
            pltpu.VMEM((GROUP, 8, tokens), F32),
            pltpu.VMEM((HEAD_DIM, tokens), BF16),
        ],
        compiler_params=params,
        cost_estimate=cost(20),
        name="values",
    )(raw_inputs, halo, state_maps, step_size, log_decay, taps, bias)

    got = lax.all_to_all(message, axis, 0, 0, tiled=True)

    skip = jnp.broadcast_to(jnp.repeat(skip_gain, HEAD_DIM)[:, None], (channels, 128))

    def local_part(first, number, previous):
        shift = lambda g: (g + first, 0)
        specs = [
            pl.BlockSpec((ROWS, tokens), shift),
            maps,
            pl.BlockSpec((GROUP, tokens), shift),
            pl.BlockSpec((GROUP, tokens), shift),
            pl.BlockSpec((ROWS, 128), shift),
        ]
        arrays = [values, state_maps, step_size, sums, skip]
        alias = {}
        if previous is not None:
            specs.append(pl.BlockSpec(memory_space=pl.ANY))
            arrays.append(previous)
            alias = {5: 0}
        return pl.pallas_call(
            functools.partial(local_kernel, chunks),
            grid=(number,),
            in_specs=specs,
            out_specs=pl.BlockSpec((ROWS, tokens), shift),
            out_shape=jax.ShapeDtypeStruct((channels, tokens), BF16),
            scratch_shapes=[pltpu.VMEM((ROWS, STATE), F32)],
            input_output_aliases=alias,
            compiler_params=params,
            cost_estimate=cost(4 * number),
            name="inside",
        )(*arrays)

    early = groups // 2
    partial = local_part(0, early, None)

    entering = pl.pallas_call(
        scan_kernel,
        in_specs=[pl.BlockSpec(memory_space=pltpu.VMEM)],
        out_specs=pl.BlockSpec(memory_space=pltpu.VMEM),
        out_shape=jax.ShapeDtypeStruct((count, 16, 128), BF16),
        cost_estimate=cost(3),
        name="scan",
    )(got)
    back = lax.all_to_all(entering, axis, 0, 0, tiled=True)

    partial = local_part(early, groups - early, partial)

    return pl.pallas_call(
        functools.partial(carried_kernel, chunks),
        grid=(groups,),
        in_specs=[
            big,
            maps,
            rows8,
            pl.BlockSpec((2 * GROUP, 16, 128), lambda g: (g, 0, 0)),
        ],
        out_specs=big,
        out_shape=jax.ShapeDtypeStruct((channels, tokens), BF16),
        input_output_aliases={0: 0},
        compiler_params=params,
        cost_estimate=cost(8),
        name="carried",
    )(partial, state_maps, lead, back)


def solution(mesh):
    axis = mesh.axis_names[0]
    return jax.shard_map(
        functools.partial(local, axis=axis),
        mesh=mesh,
        in_specs=(P(None, axis),) * 4 + (P(),) * 3,
        out_specs=P(None, axis),
        check_vma=False,
    )
```

```python
import functools

import jax
import jax.numpy as jnp
from jax import lax
from jax.experimental import pallas as pl
from jax.experimental.pallas import tpu as pltpu
from jax.sharding import PartitionSpec as P

CHUNK = 128
SEGMENT = 16
GROUP = 8
UNROLL = 8
CHUNKS_PER_STEP = 14
EARLY = 2
MIDDLE = 2
HEAD_DIM = 64
STATE = 64
ROWS = GROUP * HEAD_DIM
LOG2E = 1.4426950408889634
F32 = jnp.float32
BF16 = jnp.bfloat16


def dot_nt(a, b):
    return lax.dot_general(a, b, (((1,), (1,)), ((), ())), preferred_element_type=F32)


def chunk_sums(log_decay, chunks):
    stacked = jnp.concatenate(
        [log_decay[:, c * CHUNK : (c + 1) * CHUNK] for c in range(chunks)], axis=0
    ) * LOG2E
    row = lax.broadcasted_iota(jnp.int32, (CHUNK, CHUNK), 0)
    col = lax.broadcasted_iota(jnp.int32, (CHUNK, CHUNK), 1)
    upper = jnp.where(row <= col, 1.0, 0.0).astype(F32)
    summed = lax.dot_general(
        stacked, upper, (((1,), (0,)), ((), ())),
        precision=lax.Precision.HIGHEST, preferred_element_type=F32,
    )
    return [summed[c * GROUP : (c + 1) * GROUP] for c in range(chunks)]


def values_kernel(chunks, raw_ref, halo_ref, maps_ref, step_ref, decay_ref, taps_ref, bias_ref,
                  x_ref, sums_ref, lead_ref, msg_ref, d_scr, xd_scr):
    sums = chunk_sums(decay_ref[...], chunks)
    ends = [jnp.broadcast_to(s[:, CHUNK - 1 :], (GROUP, CHUNK)) for s in sums]
    before = jnp.zeros((GROUP, CHUNK), F32)
    for c in range(chunks):
        at = slice(c * CHUNK, (c + 1) * CHUNK)
        sums_ref[:, at] = sums[c]
        lead_ref[:, at] = jnp.exp2(before + sums[c])
        before = before + ends[c]
    after = jnp.zeros((GROUP, CHUNK), F32)
    for c in reversed(range(chunks)):
        at = slice(c * CHUNK, (c + 1) * CHUNK)
        to_end = jnp.exp2((ends[c] - sums[c]) + after) * step_ref[:, at]
        for h in range(GROUP):
            d_scr[h, :, at] = jnp.broadcast_to(to_end[h : h + 1, :], (8, CHUNK))
        after = after + ends[c]
    total = jnp.exp2(before)
    hi = total.astype(BF16).astype(F32)
    low = total - hi
    for h in range(GROUP):
        tile = jnp.concatenate(
            [jnp.broadcast_to(hi[h : h + 1], (8, CHUNK)), jnp.broadcast_to(low[h : h + 1], (8, CHUNK))], axis=0
        ).astype(BF16)
        msg_ref[2 * h, 16:, :] = tile
        msg_ref[2 * h + 1, 16:, :] = tile

    keys = maps_ref[:STATE, :]
    row = lax.broadcasted_iota(jnp.int32, (HEAD_DIM, 4 * HEAD_DIM), 0)
    col = lax.broadcasted_iota(jnp.int32, (HEAD_DIM, 4 * HEAD_DIM), 1)
    diagonal = row == lax.rem(col, HEAD_DIM)
    lane = lax.broadcasted_iota(jnp.int32, (HEAD_DIM, CHUNK), 1)
    inside = [lane >= k for k in range(4)]

    def one_head(head):
        rows = pl.ds(pl.multiple_of(head * HEAD_DIM, HEAD_DIM), HEAD_DIM)
        taps = jnp.broadcast_to(taps_ref[head, :1, :], (HEAD_DIM, 4 * HEAD_DIM))
        taps = jnp.where(diagonal, taps, 0.0)
        taps_hi = taps.astype(BF16)
        taps_low = (taps - taps_hi.astype(F32)).astype(BF16)
        left = jnp.concatenate([taps_hi, taps_low], axis=0)
        bias = jnp.broadcast_to(bias_ref[rows, :1], (HEAD_DIM, 2 * CHUNK))
        last = halo_ref[rows, :]
        prior = [None] + [pltpu.roll(last, k, 1) for k in (1, 2, 3)]
        for t in range(chunks // 2):
            columns = []
            for c in (2 * t, 2 * t + 1):
                now = raw_ref[rows, c * CHUNK : (c + 1) * CHUNK]
                rolled = [None] + [pltpu.roll(now, k, 1) for k in (1, 2, 3)]
                moved = [jnp.where(inside[k], rolled[k], prior[k]) for k in (3, 2, 1)]
                columns.append(jnp.concatenate(moved + [now], axis=0))
                prior = rolled
            at = slice(2 * t * CHUNK, 2 * (t + 1) * CHUNK)
            both = jnp.dot(left, jnp.concatenate(columns, axis=1), preferred_element_type=F32)
            half = (both[:HEAD_DIM] + both[HEAD_DIM:]) + bias
            value = half + half * jnp.tanh(half)
            x_ref[rows, at] = value.astype(BF16)
            to_end = d_scr[head, :, at]
            to_end = jnp.concatenate([to_end] * 8, axis=0)
            xd_scr[rows, at] = (value * to_end).astype(BF16)

    def body(pair, carry):
        for k in range(UNROLL):
            one_head(pair * UNROLL + k)
        return carry

    lax.fori_loop(0, GROUP // UNROLL, body, 0)
    states = dot_nt(xd_scr[...], keys).astype(BF16)
    for k in range(2 * GROUP):
        msg_ref[k, :16, :] = jnp.concatenate(
            [states[32 * k : 32 * k + 16], states[32 * k + 16 : 32 * k + 32]], axis=1
        )


def scan_kernel(got_ref, out_ref):
    entering = jnp.zeros((16, 128), F32)
    for d in range(got_ref.shape[0]):
        out_ref[d] = entering.astype(BF16)
        parts = got_ref[d, 16:, :].astype(F32)
        decay = parts[:8] + parts[8:]
        decay = jnp.concatenate([decay, decay], axis=0)
        entering = decay * entering + got_ref[d, :16, :].astype(F32)


def head_states(enter_ref):
    pieces = []
    for k in range(2 * GROUP):
        tile = enter_ref[k]
        pieces += [tile[:, :STATE], tile[:, STATE:]]
    return jnp.concatenate(pieces, axis=0)


def spread(row, count):
    return jnp.concatenate([jnp.broadcast_to(row, (16, CHUNK)).astype(BF16)] * count, axis=0)


def local_kernel(chunks, started, *refs):
    x_ref, maps_ref, step_ref, sums_ref, skip_ref = refs[:5]
    y_ref, state_scr = refs[-2:]
    if started:
        state_scr[...] = head_states(refs[5]).astype(F32)
    else:
        state_scr[...] = jnp.zeros_like(state_scr)
    jdx = lax.broadcasted_iota(jnp.int32, (CHUNK, CHUNK), 0)
    idx = lax.broadcasted_iota(jnp.int32, (CHUNK, CHUNK), 1)
    causal = idx >= jdx
    segment = lax.div(lax.broadcasted_iota(jnp.int32, (GROUP, CHUNK), 1), SEGMENT)
    segments = CHUNK // SEGMENT

    def one_chunk(c):
        at = pl.ds(pl.multiple_of(c * CHUNK, CHUNK), CHUNK)
        keys = maps_ref[:STATE, at]
        queries = maps_ref[STATE:, at]
        affinity = jnp.dot(jnp.transpose(keys), queries, preferred_element_type=F32)
        affinity = jnp.where(causal, affinity, 0.0).astype(BF16)
        sums = sums_ref[:, at]
        steps = step_ref[:, at]
        ends = jnp.broadcast_to(sums[:, CHUNK - 1 :], (GROUP, CHUNK))
        rise = jnp.exp2(sums)
        fall = jnp.exp2(ends - sums) * steps
        marks = ends
        grown = []
        for b in range(segments):
            last = (b + 1) * SEGMENT - 1
            mark = jnp.broadcast_to(sums[:, last : last + 1], (GROUP, CHUNK))
            grown.append(jnp.exp2(jnp.minimum(sums - mark, 100.0)))
            marks = jnp.where(segment == b, mark, marks)
        shrunk = jnp.exp2(marks - sums) * steps
        scaled = []
        for h in range(GROUP):
            rows = slice(h * HEAD_DIM, (h + 1) * HEAD_DIM)
            one = slice(h, h + 1)
            x = x_ref[rows, at]
            pieces = [
                affinity[b * SEGMENT : (b + 1) * SEGMENT] * spread(grown[b][one], 1)
                for b in range(segments)
            ]
            risen = queries * spread(rise[one], 4)
            stepped = x * spread(shrunk[one], 4)
            left = jnp.concatenate([stepped, state_scr[rows, :].astype(BF16)], axis=1)
            right = jnp.concatenate(pieces + [risen], axis=0)
            out = jnp.dot(left, right, preferred_element_type=F32)
            out = out + x.astype(F32) * skip_ref[one, :]
            y_ref[rows, at] = out.astype(BF16)
            scaled.append(x * spread(fall[one], 4))
        update = dot_nt(jnp.concatenate(scaled, axis=0), keys)
        for h in range(GROUP):
            rows = slice(h * HEAD_DIM, (h + 1) * HEAD_DIM)
            decay = jnp.broadcast_to(rise[h : h + 1, CHUNK - 1 :], (HEAD_DIM, STATE))
            state_scr[rows, :] = state_scr[rows, :] * decay + update[rows]

    def body(t, carry):
        for k in range(CHUNKS_PER_STEP):
            one_chunk(CHUNKS_PER_STEP * t + k)
        return carry

    lax.fori_loop(0, chunks // CHUNKS_PER_STEP, body, 0)


def carried_kernel(chunks, y_ref, maps_ref, lead_ref, enter_ref, out_ref):
    entering = head_states(enter_ref)
    for c in range(chunks // 2):
        at = slice(c * 256, (c + 1) * 256)
        queries = maps_ref[STATE:, at]
        carried = jnp.dot(entering, queries, preferred_element_type=F32)
        for h in range(GROUP):
            rows = slice(h * HEAD_DIM, (h + 1) * HEAD_DIM)
            add = carried[rows] * lead_ref[h : h + 1, at]
            out_ref[rows, at] = (y_ref[rows, at].astype(F32) + add).astype(BF16)


def local(raw_inputs, state_maps, step_size, log_decay, conv_weight, conv_bias, skip_gain, axis):
    channels, tokens = raw_inputs.shape
    heads = skip_gain.shape[0]
    groups = heads // GROUP
    chunks = tokens // CHUNK
    count = lax.axis_size(axis)

    tail = lax.ppermute(
        raw_inputs[:, tokens - 3 :], axis, [(i, i + 1) for i in range(count - 1)]
    )
    halo = jnp.pad(tail, ((0, 0), (CHUNK - 3, 0)))

    taps = 0.5 * jnp.transpose(conv_weight.reshape(4, heads, HEAD_DIM), (1, 0, 2))
    taps = taps.reshape(heads, 1, 4 * HEAD_DIM)
    bias = jnp.broadcast_to(0.5 * conv_bias[:, None], (channels, 128))

    block = lambda g: (g, 0)
    whole = lambda g: (0, 0)
    big = pl.BlockSpec((ROWS, tokens), block)
    rows8 = pl.BlockSpec((GROUP, tokens), block)
    maps = pl.BlockSpec((2 * STATE, tokens), whole)
    cost = lambda us: pl.CostEstimate(
        flops=int(us * 5e8), bytes_accessed=int(us * 1e6), transcendentals=0
    )
    params = pltpu.CompilerParams(dimension_semantics=("arbitrary",))

    values, sums, lead, message = pl.pallas_call(
        functools.partial(values_kernel, chunks),
        grid=(groups,),
        in_specs=[
            big,
            pl.BlockSpec((ROWS, CHUNK), block),
            maps,
            rows8,
            rows8,
            pl.BlockSpec((GROUP, 1, 4 * HEAD_DIM), lambda g: (g, 0, 0)),
            pl.BlockSpec((ROWS, 128), block),
        ],
        out_specs=[big, rows8, rows8, pl.BlockSpec((2 * GROUP, 32, 128), lambda g: (g, 0, 0))],
        out_shape=[
            jax.ShapeDtypeStruct((channels, tokens), BF16),
            jax.ShapeDtypeStruct((heads, tokens), F32),
            jax.ShapeDtypeStruct((heads, tokens), F32),
            jax.ShapeDtypeStruct((count, 32, 128), BF16),
        ],
        scratch_shapes=[
            pltpu.VMEM((GROUP, 8, tokens), F32),
            pltpu.VMEM((ROWS, tokens), BF16),
        ],
        compiler_params=params,
        cost_estimate=cost(20),
        name="values",
    )(raw_inputs, halo, state_maps, step_size, log_decay, taps, bias)

    got = lax.all_to_all(message, axis, 0, 0, tiled=True)

    skip = jnp.broadcast_to(skip_gain[:, None], (heads, CHUNK))

    def local_part(first, number, previous, enter=None):
        shift = lambda g: (g + first, 0)
        specs = [
            pl.BlockSpec((ROWS, tokens), shift),
            maps,
            pl.BlockSpec((GROUP, tokens), shift),
            pl.BlockSpec((GROUP, tokens), shift),
            pl.BlockSpec((GROUP, CHUNK), shift),
        ]
        arrays = [values, state_maps, step_size, sums, skip]
        alias = {}
        if enter is not None:
            specs.append(pl.BlockSpec((2 * GROUP, 16, 128), lambda g: (g + first, 0, 0)))
            arrays.append(enter)
        if previous is not None:
            alias = {len(arrays): 0}
            specs.append(pl.BlockSpec(memory_space=pl.ANY))
            arrays.append(previous)
        return pl.pallas_call(
            functools.partial(local_kernel, chunks, enter is not None),
            grid=(number,),
            in_specs=specs,
            out_specs=pl.BlockSpec((ROWS, tokens), shift),
            out_shape=jax.ShapeDtypeStruct((channels, tokens), BF16),
            scratch_shapes=[pltpu.VMEM((ROWS, STATE), F32)],
            input_output_aliases=alias,
            compiler_params=params,
            cost_estimate=cost(8 * number),
            name="inside",
        )(*arrays)

    early, middle = EARLY, EARLY + MIDDLE
    partial = local_part(0, early, None)

    entering = pl.pallas_call(
        scan_kernel,
        in_specs=[pl.BlockSpec(memory_space=pltpu.VMEM)],
        out_specs=pl.BlockSpec(memory_space=pltpu.VMEM),
        out_shape=jax.ShapeDtypeStruct((count, 16, 128), BF16),
        cost_estimate=cost(3),
        name="scan",
    )(got)
    back = lax.all_to_all(entering, axis, 0, 0, tiled=True)

    partial = local_part(early, middle - early, partial)
    partial = local_part(middle, groups - middle, partial, back)

    return pl.pallas_call(
        functools.partial(carried_kernel, chunks),
        grid=(middle,),
        in_specs=[
            big,
            maps,
            rows8,
            pl.BlockSpec((2 * GROUP, 16, 128), lambda g: (g, 0, 0)),
        ],
        out_specs=big,
        out_shape=jax.ShapeDtypeStruct((channels, tokens), BF16),
        input_output_aliases={0: 0},
        compiler_params=params,
        cost_estimate=cost(8),
        name="carried",
    )(partial, state_maps, lead, back)


def solution(mesh):
    axis = mesh.axis_names[0]
    return jax.shard_map(
        functools.partial(local, axis=axis),
        mesh=mesh,
        in_specs=(P(None, axis),) * 4 + (P(),) * 3,
        out_specs=P(None, axis),
        check_vma=False,
    )
```

```python
import functools

import jax
import jax.numpy as jnp
from jax import lax
from jax.experimental import pallas as pl
from jax.experimental.pallas import tpu as pltpu
from jax.sharding import PartitionSpec as P

CHUNK = 128
SEGMENT = 16
GROUP = 8
CHUNKS_PER_STEP = 14
EARLY = 2
MIDDLE = 2
HEAD_DIM = 64
STATE = 64
ROWS = GROUP * HEAD_DIM
LOG2E = 1.4426950408889634
F32 = jnp.float32
BF16 = jnp.bfloat16


def dot_nt(a, b):
    return lax.dot_general(a, b, (((1,), (1,)), ((), ())), preferred_element_type=F32)


def chunk_sums(log_decay, chunks):
    stacked = jnp.concatenate(
        [log_decay[:, c * CHUNK : (c + 1) * CHUNK] for c in range(chunks)], axis=0
    ) * LOG2E
    row = lax.broadcasted_iota(jnp.int32, (CHUNK, CHUNK), 0)
    col = lax.broadcasted_iota(jnp.int32, (CHUNK, CHUNK), 1)
    upper = jnp.where(row <= col, 1.0, 0.0).astype(F32)
    summed = lax.dot_general(
        stacked, upper, (((1,), (0,)), ((), ())),
        precision=lax.Precision.HIGHEST, preferred_element_type=F32,
    )
    return [summed[c * GROUP : (c + 1) * GROUP] for c in range(chunks)]


def values_kernel(chunks, raw_ref, halo_ref, maps_ref, step_ref, decay_ref, taps_ref, bias_ref,
                  x_ref, sums_ref, lead_ref, msg_ref, d_scr, xd_scr):
    sums = chunk_sums(decay_ref[...], chunks)
    ends = [jnp.broadcast_to(s[:, CHUNK - 1 :], (GROUP, CHUNK)) for s in sums]
    before = jnp.zeros((GROUP, CHUNK), F32)
    for c in range(chunks):
        at = slice(c * CHUNK, (c + 1) * CHUNK)
        sums_ref[:, at] = sums[c]
        lead_ref[:, at] = jnp.exp2(before + sums[c])
        before = before + ends[c]
    after = jnp.zeros((GROUP, CHUNK), F32)
    for c in reversed(range(chunks)):
        at = slice(c * CHUNK, (c + 1) * CHUNK)
        to_end = jnp.exp2((ends[c] - sums[c]) + after) * step_ref[:, at]
        for h in range(GROUP):
            d_scr[h, :, at] = jnp.broadcast_to(to_end[h : h + 1, :], (8, CHUNK))
        after = after + ends[c]
    total = jnp.exp2(before)
    hi = total.astype(BF16).astype(F32)
    low = total - hi
    for h in range(GROUP):
        tile = jnp.concatenate(
            [jnp.broadcast_to(hi[h : h + 1], (4, CHUNK)), jnp.broadcast_to(low[h : h + 1], (4, CHUNK))], axis=0
        ).astype(BF16)
        msg_ref[2 * h, 16:, :] = tile
        msg_ref[2 * h + 1, 16:, :] = tile

    keys = maps_ref[:STATE, :]
    row = lax.broadcasted_iota(jnp.int32, (HEAD_DIM, 4 * HEAD_DIM), 0)
    col = lax.broadcasted_iota(jnp.int32, (HEAD_DIM, 4 * HEAD_DIM), 1)
    diagonal = row == lax.rem(col, HEAD_DIM)
    lane = lax.broadcasted_iota(jnp.int32, (HEAD_DIM, CHUNK), 1)
    inside = [lane >= k for k in range(4)]

    all_taps = taps_ref[...] * 0.5
    all_bias = jnp.transpose(jnp.broadcast_to(bias_ref[...] * 0.5, (8, ROWS)))

    def one_head(head):
        rows = slice(head * HEAD_DIM, (head + 1) * HEAD_DIM)
        taps = jnp.concatenate([all_taps[k : k + 1, rows] for k in range(4)], axis=1)
        taps = jnp.broadcast_to(taps, (HEAD_DIM, 4 * HEAD_DIM))
        taps = jnp.where(diagonal, taps, 0.0)
        taps_hi = taps.astype(BF16)
        taps_low = (taps - taps_hi.astype(F32)).astype(BF16)
        left = jnp.concatenate([taps_hi, taps_low], axis=0)
        bias = jnp.broadcast_to(all_bias[rows, :1], (HEAD_DIM, 2 * CHUNK))
        last = halo_ref[rows, :]
        prior = [None] + [pltpu.roll(last, k, 1) for k in (1, 2, 3)]
        for t in range(chunks // 2):
            columns = []
            for c in (2 * t, 2 * t + 1):
                now = raw_ref[rows, c * CHUNK : (c + 1) * CHUNK]
                rolled = [None] + [pltpu.roll(now, k, 1) for k in (1, 2, 3)]
                moved = [jnp.where(inside[k], rolled[k], prior[k]) for k in (3, 2, 1)]
                columns.append(jnp.concatenate(moved + [now], axis=0))
                prior = rolled
            at = slice(2 * t * CHUNK, 2 * (t + 1) * CHUNK)
            both = jnp.dot(left, jnp.concatenate(columns, axis=1), preferred_element_type=F32)
            half = (both[:HEAD_DIM] + both[HEAD_DIM:]) + bias
            value = half + half * jnp.tanh(half)
            x_ref[rows, at] = value.astype(BF16)
            to_end = d_scr[head, :, at]
            to_end = jnp.concatenate([to_end] * 8, axis=0)
            xd_scr[rows, at] = (value * to_end).astype(BF16)

    for head in range(GROUP):
        one_head(head)
    states = dot_nt(xd_scr[...], keys).astype(BF16)
    for k in range(2 * GROUP):
        msg_ref[k, :16, :] = jnp.concatenate(
            [states[32 * k : 32 * k + 16], states[32 * k + 16 : 32 * k + 32]], axis=1
        )


def scan_kernel(got_ref, out_ref):
    entering = jnp.zeros((16, 128), F32)
    for d in range(got_ref.shape[0]):
        out_ref[d] = entering.astype(BF16)
        parts = got_ref[d, 16:, :].astype(F32)
        decay = parts + pltpu.roll(parts, 4, 0)
        decay = jnp.concatenate([decay, decay], axis=0)
        entering = decay * entering + got_ref[d, :16, :].astype(F32)


def head_states(enter_ref):
    pieces = []
    for k in range(2 * GROUP):
        tile = enter_ref[k]
        pieces += [tile[:, :STATE], tile[:, STATE:]]
    return jnp.concatenate(pieces, axis=0)


def spread(row, count):
    return jnp.concatenate([jnp.broadcast_to(row, (16, CHUNK)).astype(BF16)] * count, axis=0)


def local_kernel(chunks, started, *refs):
    x_ref, maps_ref, step_ref, sums_ref, skip_ref = refs[:5]
    y_ref, state_scr = refs[-2:]
    if started:
        state_scr[...] = head_states(refs[5]).astype(F32)
    else:
        state_scr[...] = jnp.zeros_like(state_scr)
    jdx = lax.broadcasted_iota(jnp.int32, (CHUNK, CHUNK), 0)
    idx = lax.broadcasted_iota(jnp.int32, (CHUNK, CHUNK), 1)
    causal = idx >= jdx
    segment = lax.div(lax.broadcasted_iota(jnp.int32, (GROUP, CHUNK), 1), SEGMENT)
    segments = CHUNK // SEGMENT

    def one_chunk(c):
        at = pl.ds(pl.multiple_of(c * CHUNK, CHUNK), CHUNK)
        keys = maps_ref[:STATE, at]
        queries = maps_ref[STATE:, at]
        affinity = jnp.dot(jnp.transpose(keys), queries, preferred_element_type=F32)
        affinity = jnp.where(causal, affinity, 0.0).astype(BF16)
        sums = sums_ref[:, at]
        steps = step_ref[:, at]
        ends = jnp.broadcast_to(sums[:, CHUNK - 1 :], (GROUP, CHUNK))
        rise = jnp.exp2(sums)
        fall = jnp.exp2(ends - sums) * steps
        marks = ends
        grown = []
        for b in range(segments):
            last = (b + 1) * SEGMENT - 1
            mark = jnp.broadcast_to(sums[:, last : last + 1], (GROUP, CHUNK))
            grown.append(jnp.exp2(jnp.minimum(sums - mark, 100.0)))
            marks = jnp.where(segment == b, mark, marks)
        shrunk = jnp.exp2(marks - sums) * steps
        scaled = []
        for h in range(GROUP):
            rows = slice(h * HEAD_DIM, (h + 1) * HEAD_DIM)
            one = slice(h, h + 1)
            x = x_ref[rows, at]
            pieces = [
                affinity[b * SEGMENT : (b + 1) * SEGMENT] * spread(grown[b][one], 1)
                for b in range(segments)
            ]
            risen = queries * spread(rise[one], 4)
            stepped = x * spread(shrunk[one], 4)
            left = jnp.concatenate([stepped, state_scr[rows, :].astype(BF16)], axis=1)
            right = jnp.concatenate(pieces + [risen], axis=0)
            out = jnp.dot(left, right, preferred_element_type=F32)
            out = out + x.astype(F32) * skip_ref[one, :]
            y_ref[rows, at] = out.astype(BF16)
            scaled.append(x * spread(fall[one], 4))
        update = dot_nt(jnp.concatenate(scaled, axis=0), keys)
        for h in range(GROUP):
            rows = slice(h * HEAD_DIM, (h + 1) * HEAD_DIM)
            decay = jnp.broadcast_to(rise[h : h + 1, CHUNK - 1 :], (HEAD_DIM, STATE))
            state_scr[rows, :] = state_scr[rows, :] * decay + update[rows]

    def body(t, carry):
        for k in range(CHUNKS_PER_STEP):
            one_chunk(CHUNKS_PER_STEP * t + k)
        return carry

    lax.fori_loop(0, chunks // CHUNKS_PER_STEP, body, 0)


def carried_group(chunks, y_ref, maps_ref, lead_ref, enter_ref, out_ref):
    entering = head_states(enter_ref)
    for c in range(chunks // 2):
        at = slice(c * 256, (c + 1) * 256)
        carried = jnp.dot(entering, maps_ref[STATE:, at], preferred_element_type=F32)
        for h in range(GROUP):
            rows = slice(h * HEAD_DIM, (h + 1) * HEAD_DIM)
            add = carried[rows] * lead_ref[h : h + 1, at]
            out_ref[rows, at] = (y_ref[rows, at].astype(F32) + add).astype(BF16)


def last_kernel(chunks, late, x_ref, maps_ref, step_ref, sums_ref, skip_ref, enter_ref, y_ref, lead_ref,
                out_ref, state_scr):
    g = pl.program_id(0)
    is_late = (lax.rem(g, 2) == 0) & (g < 2 * late)

    @pl.when(is_late)
    def _():
        local_kernel(chunks, True, x_ref, maps_ref, step_ref, sums_ref, skip_ref, enter_ref, out_ref, state_scr)

    @pl.when(jnp.logical_not(is_late))
    def _():
        carried_group(chunks, y_ref, maps_ref, lead_ref, enter_ref, out_ref)


def local(raw_inputs, state_maps, step_size, log_decay, conv_weight, conv_bias, skip_gain, axis):
    channels, tokens = raw_inputs.shape
    heads = skip_gain.shape[0]
    groups = heads // GROUP
    chunks = tokens // CHUNK
    count = lax.axis_size(axis)

    tail = lax.ppermute(
        raw_inputs[:, tokens - 3 :], axis, [(i, i + 1) for i in range(count - 1)]
    )
    halo = jnp.pad(tail, ((0, 0), (CHUNK - 3, 0)))

    block = lambda g: (g, 0)
    whole = lambda g: (0, 0)
    big = pl.BlockSpec((ROWS, tokens), block)
    rows8 = pl.BlockSpec((GROUP, tokens), block)
    maps = pl.BlockSpec((2 * STATE, tokens), whole)
    cost = lambda us: pl.CostEstimate(
        flops=int(us * 5e8), bytes_accessed=int(us * 1e6), transcendentals=0
    )
    params = pltpu.CompilerParams(dimension_semantics=("arbitrary",))

    values, sums, lead, message = pl.pallas_call(
        functools.partial(values_kernel, chunks),
        grid=(groups,),
        in_specs=[
            big,
            pl.BlockSpec((ROWS, CHUNK), block),
            maps,
            rows8,
            rows8,
            pl.BlockSpec((4, ROWS), lambda g: (0, g)),
            pl.BlockSpec((1, ROWS), lambda g: (0, g)),
        ],
        out_specs=[big, rows8, rows8, pl.BlockSpec((2 * GROUP, 24, 128), lambda g: (g, 0, 0))],
        out_shape=[
            jax.ShapeDtypeStruct((channels, tokens), BF16),
            jax.ShapeDtypeStruct((heads, tokens), F32),
            jax.ShapeDtypeStruct((heads, tokens), F32),
            jax.ShapeDtypeStruct((count, 24, 128), BF16),
        ],
        scratch_shapes=[
            pltpu.VMEM((GROUP, 8, tokens), F32),
            pltpu.VMEM((ROWS, tokens), BF16),
        ],
        compiler_params=params,
        cost_estimate=cost(20),
        name="values",
    )(raw_inputs, halo, state_maps, step_size, log_decay, conv_weight, conv_bias.reshape(1, channels))

    got = lax.all_to_all(message, axis, 0, 0, tiled=True)

    skip = jnp.broadcast_to(skip_gain[:, None], (heads, CHUNK))

    def local_part(first, number, previous, enter=None):
        shift = lambda g: (g + first, 0)
        specs = [
            pl.BlockSpec((ROWS, tokens), shift),
            maps,
            pl.BlockSpec((GROUP, tokens), shift),
            pl.BlockSpec((GROUP, tokens), shift),
            pl.BlockSpec((GROUP, CHUNK), shift),
        ]
        arrays = [values, state_maps, step_size, sums, skip]
        alias = {}
        if enter is not None:
            specs.append(pl.BlockSpec((2 * GROUP, 16, 128), lambda g: (g + first, 0, 0)))
            arrays.append(enter)
        if previous is not None:
            alias = {len(arrays): 0}
            specs.append(pl.BlockSpec(memory_space=pl.ANY))
            arrays.append(previous)
        return pl.pallas_call(
            functools.partial(local_kernel, chunks, enter is not None),
            grid=(number,),
            in_specs=specs,
            out_specs=pl.BlockSpec((ROWS, tokens), shift),
            out_shape=jax.ShapeDtypeStruct((channels, tokens), BF16),
            scratch_shapes=[pltpu.VMEM((ROWS, STATE), F32)],
            input_output_aliases=alias,
            compiler_params=params,
            cost_estimate=cost(8 * number),
            name="inside",
        )(*arrays)

    early, middle = EARLY, EARLY + MIDDLE
    partial = local_part(0, early, None)

    entering = pl.pallas_call(
        scan_kernel,
        in_specs=[pl.BlockSpec(memory_space=pltpu.VMEM)],
        out_specs=pl.BlockSpec(memory_space=pltpu.VMEM),
        out_shape=jax.ShapeDtypeStruct((count, 16, 128), BF16),
        cost_estimate=cost(3),
        name="scan",
    )(got)
    back = lax.all_to_all(entering, axis, 0, 0, tiled=True)

    partial = local_part(early, middle - early, partial)
    late = groups - middle

    def late_group(g):
        return middle + jnp.minimum((g + 1) // 2, late - 1)

    def early_group(g):
        return jnp.where(g >= 2 * late, g - late, jnp.maximum(g - 1, 0) // 2)

    def own_group(g):
        return jnp.where((g % 2 == 0) & (g < 2 * late), late_group(g), early_group(g))

    at_late = lambda g: (late_group(g), 0)
    at_early = lambda g: (early_group(g), 0)
    return pl.pallas_call(
        functools.partial(last_kernel, chunks, late),
        grid=(groups,),
        in_specs=[
            pl.BlockSpec((ROWS, tokens), at_late),
            maps,
            pl.BlockSpec((GROUP, tokens), at_late),
            pl.BlockSpec((GROUP, tokens), at_late),
            pl.BlockSpec((GROUP, CHUNK), at_late),
            pl.BlockSpec((2 * GROUP, 16, 128), lambda g: (own_group(g), 0, 0)),
            pl.BlockSpec((ROWS, tokens), at_early),
            pl.BlockSpec((GROUP, tokens), at_early),
        ],
        out_specs=pl.BlockSpec((ROWS, tokens), lambda g: (own_group(g), 0)),
        out_shape=jax.ShapeDtypeStruct((channels, tokens), BF16),
        scratch_shapes=[pltpu.VMEM((ROWS, STATE), F32)],
        input_output_aliases={6: 0},
        compiler_params=params,
        cost_estimate=cost(20),
        name="last",
    )(values, state_maps, step_size, sums, skip, back, partial, lead)


def solution(mesh):
    axis = mesh.axis_names[0]
    return jax.shard_map(
        functools.partial(local, axis=axis),
        mesh=mesh,
        in_specs=(P(None, axis),) * 4 + (P(),) * 3,
        out_specs=P(None, axis),
        check_vma=False,
    )
```

```python
import functools

import jax
import jax.numpy as jnp
from jax import lax
from jax.experimental import pallas as pl
from jax.experimental.pallas import tpu as pltpu
from jax.sharding import PartitionSpec as P

CHUNK = 128
SEGMENT = 32
GROUP = 8
CHUNKS_PER_STEP = 14
EARLY = 2
MIDDLE = 2
HEAD_DIM = 64
STATE = 64
ROWS = GROUP * HEAD_DIM
LOG2E = 1.4426950408889634
F32 = jnp.float32
BF16 = jnp.bfloat16


def dot_nt(a, b):
    return lax.dot_general(a, b, (((1,), (1,)), ((), ())), preferred_element_type=F32)


def chunk_sums(log_decay, chunks):
    stacked = jnp.concatenate(
        [log_decay[:, c * CHUNK : (c + 1) * CHUNK] for c in range(chunks)], axis=0
    ) * LOG2E
    row = lax.broadcasted_iota(jnp.int32, (CHUNK, CHUNK), 0)
    col = lax.broadcasted_iota(jnp.int32, (CHUNK, CHUNK), 1)
    upper = jnp.where(row <= col, 1.0, 0.0).astype(F32)
    summed = lax.dot_general(
        stacked, upper, (((1,), (0,)), ((), ())),
        precision=lax.Precision.HIGHEST, preferred_element_type=F32,
    )
    return [summed[c * GROUP : (c + 1) * GROUP] for c in range(chunks)]


def values_kernel(chunks, raw_ref, halo_ref, maps_ref, step_ref, decay_ref, taps_ref, bias_ref,
                  x_ref, sums_ref, lead_ref, msg_ref, d_scr, xd_scr):
    sums = chunk_sums(decay_ref[...], chunks)
    ends = [jnp.broadcast_to(s[:, CHUNK - 1 :], (GROUP, CHUNK)) for s in sums]
    before = jnp.zeros((GROUP, CHUNK), F32)
    for c in range(chunks):
        at = slice(c * CHUNK, (c + 1) * CHUNK)
        sums_ref[:, at] = sums[c]
        lead_ref[:, at] = jnp.exp2(before + sums[c])
        before = before + ends[c]
    after = jnp.zeros((GROUP, CHUNK), F32)
    for c in reversed(range(chunks)):
        at = slice(c * CHUNK, (c + 1) * CHUNK)
        to_end = jnp.exp2((ends[c] - sums[c]) + after) * step_ref[:, at]
        for h in range(GROUP):
            d_scr[h, :, at] = jnp.broadcast_to(to_end[h : h + 1, :], (8, CHUNK))
        after = after + ends[c]
    total = jnp.exp2(before)
    hi = total.astype(BF16).astype(F32)
    low = total - hi
    for h in range(GROUP):
        tile = jnp.concatenate(
            [jnp.broadcast_to(hi[h : h + 1], (4, CHUNK)), jnp.broadcast_to(low[h : h + 1], (4, CHUNK))], axis=0
        ).astype(BF16)
        msg_ref[2 * h, 16:, :] = tile
        msg_ref[2 * h + 1, 16:, :] = tile

    keys = maps_ref[:STATE, :]
    row = lax.broadcasted_iota(jnp.int32, (HEAD_DIM, 4 * HEAD_DIM), 0)
    col = lax.broadcasted_iota(jnp.int32, (HEAD_DIM, 4 * HEAD_DIM), 1)
    diagonal = row == lax.rem(col, HEAD_DIM)
    lane = lax.broadcasted_iota(jnp.int32, (HEAD_DIM, CHUNK), 1)
    inside = [lane >= k for k in range(4)]

    all_taps = taps_ref[...] * 0.5
    all_bias = jnp.transpose(jnp.broadcast_to(bias_ref[...] * 0.5, (8, ROWS)))

    def one_head(head):
        rows = slice(head * HEAD_DIM, (head + 1) * HEAD_DIM)
        taps = jnp.concatenate([all_taps[k : k + 1, rows] for k in range(4)], axis=1)
        taps = jnp.broadcast_to(taps, (HEAD_DIM, 4 * HEAD_DIM))
        taps = jnp.where(diagonal, taps, 0.0)
        taps_hi = taps.astype(BF16)
        taps_low = (taps - taps_hi.astype(F32)).astype(BF16)
        left = jnp.concatenate([taps_hi, taps_low], axis=0)
        bias = jnp.broadcast_to(all_bias[rows, :1], (HEAD_DIM, 2 * CHUNK))
        last = jnp.concatenate([halo_ref[rows, :], jnp.zeros((HEAD_DIM, CHUNK - 3), BF16)], axis=1)
        prior = [None, pltpu.roll(last, CHUNK - 2, 1), pltpu.roll(last, CHUNK - 1, 1), last]
        for t in range(chunks // 2):
            columns = []
            for c in (2 * t, 2 * t + 1):
                now = raw_ref[rows, c * CHUNK : (c + 1) * CHUNK]
                rolled = [None] + [pltpu.roll(now, k, 1) for k in (1, 2, 3)]
                moved = [jnp.where(inside[k], rolled[k], prior[k]) for k in (3, 2, 1)]
                columns.append(jnp.concatenate(moved + [now], axis=0))
                prior = rolled
            at = slice(2 * t * CHUNK, 2 * (t + 1) * CHUNK)
            both = jnp.dot(left, jnp.concatenate(columns, axis=1), preferred_element_type=F32)
            half = (both[:HEAD_DIM] + both[HEAD_DIM:]) + bias
            value = half + half * jnp.tanh(half)
            x_ref[rows, at] = value.astype(BF16)
            to_end = d_scr[head, :, at]
            to_end = jnp.concatenate([to_end] * 8, axis=0)
            xd_scr[rows, at] = (value * to_end).astype(BF16)

    for head in range(GROUP):
        one_head(head)
    states = dot_nt(xd_scr[...], keys).astype(BF16)
    for k in range(2 * GROUP):
        msg_ref[k, :16, :] = jnp.concatenate(
            [states[32 * k : 32 * k + 16], states[32 * k + 16 : 32 * k + 32]], axis=1
        )


def scan_kernel(got_ref, out_ref):
    entering = jnp.zeros((16, 128), F32)
    for d in range(got_ref.shape[0]):
        out_ref[d] = entering.astype(BF16)
        parts = got_ref[d, 16:, :].astype(F32)
        decay = parts + pltpu.roll(parts, 4, 0)
        decay = jnp.concatenate([decay, decay], axis=0)
        entering = decay * entering + got_ref[d, :16, :].astype(F32)


def head_states(enter_ref):
    pieces = []
    for k in range(2 * GROUP):
        tile = enter_ref[k]
        pieces += [tile[:, :STATE], tile[:, STATE:]]
    return jnp.concatenate(pieces, axis=0)


def spread(row, count):
    return jnp.concatenate([jnp.broadcast_to(row, (16, CHUNK)).astype(BF16)] * count, axis=0)


def local_kernel(chunks, started, group_of, *refs):
    x_ref, maps_ref, step_ref, sums_ref, skip_ref = refs[:5]
    y_ref, state_scr = refs[-2:]
    first_head = group_of(pl.program_id(0)) * GROUP
    if started:
        state_scr[...] = head_states(refs[5]).astype(F32)
    else:
        state_scr[...] = jnp.zeros_like(state_scr)
    jdx = lax.broadcasted_iota(jnp.int32, (CHUNK, CHUNK), 0)
    idx = lax.broadcasted_iota(jnp.int32, (CHUNK, CHUNK), 1)
    causal = idx >= jdx
    segment = lax.div(lax.broadcasted_iota(jnp.int32, (GROUP, CHUNK), 1), SEGMENT)
    segments = CHUNK // SEGMENT

    def one_chunk(c):
        at = pl.ds(pl.multiple_of(c * CHUNK, CHUNK), CHUNK)
        keys = maps_ref[:STATE, at]
        queries = maps_ref[STATE:, at]
        affinity = jnp.dot(jnp.transpose(keys), queries, preferred_element_type=F32)
        affinity = jnp.where(causal, affinity, 0.0).astype(BF16)
        sums = sums_ref[:, at]
        steps = step_ref[:, at]
        ends = jnp.broadcast_to(sums[:, CHUNK - 1 :], (GROUP, CHUNK))
        rise = jnp.exp2(sums)
        fall = jnp.exp2(ends - sums) * steps
        marks = ends
        grown = []
        for b in range(segments):
            last = (b + 1) * SEGMENT - 1
            mark = jnp.broadcast_to(sums[:, last : last + 1], (GROUP, CHUNK))
            grown.append(jnp.exp2(jnp.minimum(sums - mark, 100.0)))
            marks = jnp.where(segment == b, mark, marks)
        shrunk = jnp.exp2(marks - sums) * steps
        scaled = []
        for h in range(GROUP):
            rows = slice(h * HEAD_DIM, (h + 1) * HEAD_DIM)
            one = slice(h, h + 1)
            x = x_ref[rows, at]
            pieces = [
                affinity[b * SEGMENT : (b + 1) * SEGMENT] * spread(grown[b][one], SEGMENT // 16)
                for b in range(segments)
            ]
            risen = queries * spread(rise[one], 4)
            stepped = x * spread(shrunk[one], 4)
            left = jnp.concatenate([stepped, state_scr[rows, :].astype(BF16)], axis=1)
            right = jnp.concatenate(pieces + [risen], axis=0)
            out = jnp.dot(left, right, preferred_element_type=F32)
            out = out + x.astype(F32) * skip_ref[first_head + h]
            y_ref[rows, at] = out.astype(BF16)
            scaled.append(x * spread(fall[one], 4))
        update = dot_nt(jnp.concatenate(scaled, axis=0), keys)
        for h in range(GROUP):
            rows = slice(h * HEAD_DIM, (h + 1) * HEAD_DIM)
            decay = jnp.broadcast_to(rise[h : h + 1, CHUNK - 1 :], (HEAD_DIM, STATE))
            state_scr[rows, :] = state_scr[rows, :] * decay + update[rows]

    def body(t, carry):
        for k in range(CHUNKS_PER_STEP):
            one_chunk(CHUNKS_PER_STEP * t + k)
        return carry

    lax.fori_loop(0, chunks // CHUNKS_PER_STEP, body, 0)


def carried_group(chunks, y_ref, maps_ref, lead_ref, enter_ref, out_ref):
    entering = head_states(enter_ref)
    for c in range(chunks // 2):
        at = slice(c * 256, (c + 1) * 256)
        carried = jnp.dot(entering, maps_ref[STATE:, at], preferred_element_type=F32)
        for h in range(GROUP):
            rows = slice(h * HEAD_DIM, (h + 1) * HEAD_DIM)
            add = carried[rows] * lead_ref[h : h + 1, at]
            out_ref[rows, at] = (y_ref[rows, at].astype(F32) + add).astype(BF16)


def last_kernel(chunks, late, late_group, x_ref, maps_ref, step_ref, sums_ref, skip_ref, enter_ref, y_ref, lead_ref,
                out_ref, state_scr):
    g = pl.program_id(0)
    is_late = (lax.rem(g, 2) == 0) & (g < 2 * late)

    @pl.when(is_late)
    def _():
        local_kernel(chunks, True, late_group, x_ref, maps_ref, step_ref, sums_ref, skip_ref, enter_ref, out_ref, state_scr)

    @pl.when(jnp.logical_not(is_late))
    def _():
        carried_group(chunks, y_ref, maps_ref, lead_ref, enter_ref, out_ref)


def local(raw_inputs, state_maps, step_size, log_decay, conv_weight, conv_bias, skip_gain, axis):
    channels, tokens = raw_inputs.shape
    heads = skip_gain.shape[0]
    groups = heads // GROUP
    chunks = tokens // CHUNK
    count = lax.axis_size(axis)

    tail = lax.ppermute(
        raw_inputs[:, tokens - 3 :], axis, [(i, i + 1) for i in range(count - 1)]
    )

    block = lambda g: (g, 0)
    whole = lambda g: (0, 0)
    big = pl.BlockSpec((ROWS, tokens), block)
    rows8 = pl.BlockSpec((GROUP, tokens), block)
    maps = pl.BlockSpec((2 * STATE, tokens), whole)
    cost = lambda us: pl.CostEstimate(
        flops=int(us * 5e8), bytes_accessed=int(us * 1e6), transcendentals=0
    )
    params = pltpu.CompilerParams(dimension_semantics=("arbitrary",))
    packed = pltpu.CompilerParams(
        dimension_semantics=("arbitrary",)
    )

    values, sums, lead, message = pl.pallas_call(
        functools.partial(values_kernel, chunks),
        grid=(groups,),
        in_specs=[
            big,
            pl.BlockSpec((ROWS, 3), block),
            maps,
            rows8,
            rows8,
            pl.BlockSpec((4, ROWS), lambda g: (0, g)),
            pl.BlockSpec((1, ROWS), lambda g: (0, g)),
        ],
        out_specs=[big, rows8, rows8, pl.BlockSpec((2 * GROUP, 24, 128), lambda g: (g, 0, 0))],
        out_shape=[
            jax.ShapeDtypeStruct((channels, tokens), BF16),
            jax.ShapeDtypeStruct((heads, tokens), F32),
            jax.ShapeDtypeStruct((heads, tokens), F32),
            jax.ShapeDtypeStruct((count, 24, 128), BF16),
        ],
        scratch_shapes=[
            pltpu.VMEM((GROUP, 8, tokens), F32),
            pltpu.VMEM((ROWS, tokens), BF16),
        ],
        compiler_params=params,
        cost_estimate=cost(20),
        name="values",
    )(raw_inputs, tail, state_maps, step_size, log_decay, conv_weight, conv_bias.reshape(1, channels))

    got = lax.all_to_all(message, axis, 0, 0, tiled=True)


    scalars = pl.BlockSpec(memory_space=pltpu.SMEM)

    def local_part(first, number, previous, enter=None):
        shift = lambda g: (g + first, 0)
        specs = [
            pl.BlockSpec((ROWS, tokens), shift),
            maps,
            pl.BlockSpec((GROUP, tokens), shift),
            pl.BlockSpec((GROUP, tokens), shift),
            scalars,
        ]
        arrays = [values, state_maps, step_size, sums, skip_gain]
        alias = {}
        if enter is not None:
            specs.append(pl.BlockSpec((2 * GROUP, 16, 128), lambda g: (g + first, 0, 0)))
            arrays.append(enter)
        if previous is not None:
            alias = {len(arrays): 0}
            specs.append(pl.BlockSpec(memory_space=pl.ANY))
            arrays.append(previous)
        return pl.pallas_call(
            functools.partial(local_kernel, chunks, enter is not None, lambda g: g + first),
            grid=(number,),
            in_specs=specs,
            out_specs=pl.BlockSpec((ROWS, tokens), shift),
            out_shape=jax.ShapeDtypeStruct((channels, tokens), BF16),
            scratch_shapes=[pltpu.VMEM((ROWS, STATE), F32)],
            input_output_aliases=alias,
            compiler_params=packed,
            cost_estimate=cost(8 * number),
            name="inside",
        )(*arrays)

    early, middle = EARLY, EARLY + MIDDLE
    partial = local_part(0, early, None)

    entering = pl.pallas_call(
        scan_kernel,
        in_specs=[pl.BlockSpec(memory_space=pltpu.VMEM)],
        out_specs=pl.BlockSpec(memory_space=pltpu.VMEM),
        out_shape=jax.ShapeDtypeStruct((count, 16, 128), BF16),
        cost_estimate=cost(3),
        name="scan",
    )(got)
    back = lax.all_to_all(entering, axis, 0, 0, tiled=True)

    partial = local_part(early, middle - early, partial)
    late = groups - middle

    def late_group(g):
        return middle + jnp.minimum((g + 1) // 2, late - 1)

    def early_group(g):
        return jnp.where(g >= 2 * late, g - late, jnp.maximum(g - 1, 0) // 2)

    def own_group(g):
        return jnp.where((g % 2 == 0) & (g < 2 * late), late_group(g), early_group(g))

    at_late = lambda g: (late_group(g), 0)
    at_early = lambda g: (early_group(g), 0)
    return pl.pallas_call(
        functools.partial(last_kernel, chunks, late, late_group),
        grid=(groups,),
        in_specs=[
            pl.BlockSpec((ROWS, tokens), at_late),
            maps,
            pl.BlockSpec((GROUP, tokens), at_late),
            pl.BlockSpec((GROUP, tokens), at_late),
            scalars,
            pl.BlockSpec((2 * GROUP, 16, 128), lambda g: (own_group(g), 0, 0)),
            pl.BlockSpec((ROWS, tokens), at_early),
            pl.BlockSpec((GROUP, tokens), at_early),
        ],
        out_specs=pl.BlockSpec((ROWS, tokens), lambda g: (own_group(g), 0)),
        out_shape=jax.ShapeDtypeStruct((channels, tokens), BF16),
        scratch_shapes=[pltpu.VMEM((ROWS, STATE), F32)],
        input_output_aliases={6: 0},
        compiler_params=packed,
        cost_estimate=cost(20),
        name="last",
    )(values, state_maps, step_size, sums, skip_gain, back, partial, lead)


def solution(mesh):
    axis = mesh.axis_names[0]
    return jax.shard_map(
        functools.partial(local, axis=axis),
        mesh=mesh,
        in_specs=(P(None, axis),) * 4 + (P(),) * 3,
        out_specs=P(None, axis),
        check_vma=False,
    )
```

```python
import functools

import jax
import jax.numpy as jnp
from jax import lax
from jax.experimental import pallas as pl
from jax.experimental.pallas import tpu as pltpu
from jax.sharding import PartitionSpec as P

CHUNK = 128
SEGMENT = 32
GROUP = 8
CHUNKS_PER_STEP = 14
EARLY = 3
MIDDLE = 2
HEAD_DIM = 64
STATE = 64
ROWS = GROUP * HEAD_DIM
LOG2E = 1.4426950408889634
F32 = jnp.float32
BF16 = jnp.bfloat16


def dot_nt(a, b):
    return lax.dot_general(a, b, (((1,), (1,)), ((), ())), preferred_element_type=F32)


def chunk_sums(log_decay, chunks):
    stacked = jnp.concatenate(
        [log_decay[:, c * CHUNK : (c + 1) * CHUNK] for c in range(chunks)], axis=0
    ) * LOG2E
    row = lax.broadcasted_iota(jnp.int32, (CHUNK, CHUNK), 0)
    col = lax.broadcasted_iota(jnp.int32, (CHUNK, CHUNK), 1)
    upper = jnp.where(row <= col, 1.0, 0.0).astype(F32)
    summed = lax.dot_general(
        stacked, upper, (((1,), (0,)), ((), ())),
        precision=lax.Precision.HIGHEST, preferred_element_type=F32,
    )
    return [summed[c * GROUP : (c + 1) * GROUP] for c in range(chunks)]


def values_kernel(chunks, raw_ref, halo_ref, maps_ref, step_ref, decay_ref, taps_ref, bias_ref,
                  x_ref, sums_ref, lead_ref, msg_ref, d_scr, xd_scr):
    sums = chunk_sums(decay_ref[...], chunks)
    ends = [jnp.broadcast_to(s[:, CHUNK - 1 :], (GROUP, CHUNK)) for s in sums]
    before = jnp.zeros((GROUP, CHUNK), F32)
    for c in range(chunks):
        at = slice(c * CHUNK, (c + 1) * CHUNK)
        sums_ref[:, at] = sums[c]
        lead_ref[:, at] = jnp.exp2(before + sums[c])
        before = before + ends[c]
    after = jnp.zeros((GROUP, CHUNK), F32)
    for c in reversed(range(chunks)):
        at = slice(c * CHUNK, (c + 1) * CHUNK)
        to_end = jnp.exp2((ends[c] - sums[c]) + after) * step_ref[:, at]
        for h in range(GROUP):
            d_scr[h, :, at] = jnp.broadcast_to(to_end[h : h + 1, :], (8, CHUNK))
        after = after + ends[c]
    total = jnp.exp2(before)
    hi = total.astype(BF16).astype(F32)
    low = total - hi
    for h in range(GROUP):
        tile = jnp.concatenate(
            [jnp.broadcast_to(hi[h : h + 1], (4, CHUNK)), jnp.broadcast_to(low[h : h + 1], (4, CHUNK))], axis=0
        ).astype(BF16)
        msg_ref[2 * h, 16:, :] = tile
        msg_ref[2 * h + 1, 16:, :] = tile

    keys = maps_ref[:STATE, :]
    row = lax.broadcasted_iota(jnp.int32, (HEAD_DIM, 4 * HEAD_DIM), 0)
    col = lax.broadcasted_iota(jnp.int32, (HEAD_DIM, 4 * HEAD_DIM), 1)
    diagonal = row == lax.rem(col, HEAD_DIM)
    lane = lax.broadcasted_iota(jnp.int32, (HEAD_DIM, CHUNK), 1)
    inside = [lane >= k for k in range(4)]

    all_taps = taps_ref[...] * 0.5
    all_bias = jnp.transpose(jnp.broadcast_to(bias_ref[...] * 0.5, (8, ROWS)))

    def one_head(head):
        rows = slice(head * HEAD_DIM, (head + 1) * HEAD_DIM)
        taps = jnp.concatenate([all_taps[k : k + 1, rows] for k in range(4)], axis=1)
        taps = jnp.broadcast_to(taps, (HEAD_DIM, 4 * HEAD_DIM))
        taps = jnp.where(diagonal, taps, 0.0)
        taps_hi = taps.astype(BF16)
        taps_low = (taps - taps_hi.astype(F32)).astype(BF16)
        left = jnp.concatenate([taps_hi, taps_low], axis=0)
        bias = jnp.broadcast_to(all_bias[rows, :1], (HEAD_DIM, 2 * CHUNK))
        last = jnp.concatenate([halo_ref[rows, :], jnp.zeros((HEAD_DIM, CHUNK - 3), BF16)], axis=1)
        prior = [None, pltpu.roll(last, CHUNK - 2, 1), pltpu.roll(last, CHUNK - 1, 1), last]
        for t in range(chunks // 2):
            columns = []
            for c in (2 * t, 2 * t + 1):
                now = raw_ref[rows, c * CHUNK : (c + 1) * CHUNK]
                rolled = [None] + [pltpu.roll(now, k, 1) for k in (1, 2, 3)]
                moved = [jnp.where(inside[k], rolled[k], prior[k]) for k in (3, 2, 1)]
                columns.append(jnp.concatenate(moved + [now], axis=0))
                prior = rolled
            at = slice(2 * t * CHUNK, 2 * (t + 1) * CHUNK)
            both = jnp.dot(left, jnp.concatenate(columns, axis=1), preferred_element_type=F32)
            half = (both[:HEAD_DIM] + both[HEAD_DIM:]) + bias
            value = half + half * jnp.tanh(half)
            x_ref[rows, at] = value.astype(BF16)
            to_end = d_scr[head, :, at]
            to_end = jnp.concatenate([to_end] * 8, axis=0)
            xd_scr[rows, at] = (value * to_end).astype(BF16)

    for head in range(GROUP):
        one_head(head)
    states = dot_nt(xd_scr[...], keys).astype(BF16)
    for k in range(2 * GROUP):
        msg_ref[k, :16, :] = jnp.concatenate(
            [states[32 * k : 32 * k + 16], states[32 * k + 16 : 32 * k + 32]], axis=1
        )


def scan_kernel(got_ref, out_ref):
    entering = jnp.zeros((16, 128), F32)
    for d in range(got_ref.shape[0]):
        out_ref[d] = entering.astype(BF16)
        parts = got_ref[d, 16:, :].astype(F32)
        decay = parts + pltpu.roll(parts, 4, 0)
        decay = jnp.concatenate([decay, decay], axis=0)
        entering = decay * entering + got_ref[d, :16, :].astype(F32)


def head_states(enter_ref):
    pieces = []
    for k in range(2 * GROUP):
        tile = enter_ref[k]
        pieces += [tile[:, :STATE], tile[:, STATE:]]
    return jnp.concatenate(pieces, axis=0)


def spread(row, count):
    return jnp.concatenate([jnp.broadcast_to(row, (16, CHUNK)).astype(BF16)] * count, axis=0)


def local_kernel(chunks, started, group_of, *refs):
    x_ref, maps_ref, step_ref, sums_ref, skip_ref = refs[:5]
    y_ref, state_scr = refs[-2:]
    first_head = group_of(pl.program_id(0)) * GROUP
    if started:
        state_scr[...] = head_states(refs[5]).astype(F32)
    else:
        state_scr[...] = jnp.zeros_like(state_scr)
    jdx = lax.broadcasted_iota(jnp.int32, (CHUNK, CHUNK), 0)
    idx = lax.broadcasted_iota(jnp.int32, (CHUNK, CHUNK), 1)
    causal = idx >= jdx
    segment = lax.div(lax.broadcasted_iota(jnp.int32, (GROUP, CHUNK), 1), SEGMENT)
    segments = CHUNK // SEGMENT

    def one_chunk(c):
        at = pl.ds(pl.multiple_of(c * CHUNK, CHUNK), CHUNK)
        keys = maps_ref[:STATE, at]
        queries = maps_ref[STATE:, at]
        affinity = jnp.dot(jnp.transpose(keys), queries, preferred_element_type=F32)
        affinity = jnp.where(causal, affinity, 0.0).astype(BF16)
        sums = sums_ref[:, at]
        steps = step_ref[:, at]
        ends = jnp.broadcast_to(sums[:, CHUNK - 1 :], (GROUP, CHUNK))
        rise = jnp.exp2(sums)
        fall = jnp.exp2(ends - sums) * steps
        marks = ends
        grown = []
        for b in range(segments):
            last = (b + 1) * SEGMENT - 1
            mark = jnp.broadcast_to(sums[:, last : last + 1], (GROUP, CHUNK))
            grown.append(jnp.exp2(jnp.minimum(sums - mark, 100.0)))
            marks = jnp.where(segment == b, mark, marks)
        shrunk = jnp.exp2(marks - sums) * steps
        scaled = []
        for h in range(GROUP):
            rows = slice(h * HEAD_DIM, (h + 1) * HEAD_DIM)
            one = slice(h, h + 1)
            x = x_ref[rows, at]
            pieces = [
                affinity[b * SEGMENT : (b + 1) * SEGMENT] * spread(grown[b][one], SEGMENT // 16)
                for b in range(segments)
            ]
            risen = queries * spread(rise[one], 4)
            stepped = x * spread(shrunk[one], 4)
            left = jnp.concatenate([stepped, state_scr[rows, :].astype(BF16)], axis=1)
            right = jnp.concatenate(pieces + [risen], axis=0)
            out = jnp.dot(left, right, preferred_element_type=F32)
            out = out + x.astype(F32) * skip_ref[first_head + h]
            y_ref[rows, at] = out.astype(BF16)
            scaled.append(x * spread(fall[one], 4))
        update = dot_nt(jnp.concatenate(scaled, axis=0), keys)
        for h in range(GROUP):
            rows = slice(h * HEAD_DIM, (h + 1) * HEAD_DIM)
            decay = jnp.broadcast_to(rise[h : h + 1, CHUNK - 1 :], (HEAD_DIM, STATE))
            state_scr[rows, :] = state_scr[rows, :] * decay + update[rows]

    def body(t, carry):
        for k in range(CHUNKS_PER_STEP):
            one_chunk(CHUNKS_PER_STEP * t + k)
        return carry

    lax.fori_loop(0, chunks // CHUNKS_PER_STEP, body, 0)


def carried_group(chunks, y_ref, maps_ref, lead_ref, enter_ref, out_ref):
    entering = head_states(enter_ref)
    for c in range(chunks // 2):
        at = slice(c * 256, (c + 1) * 256)
        carried = jnp.dot(entering, maps_ref[STATE:, at], preferred_element_type=F32)
        for h in range(GROUP):
            rows = slice(h * HEAD_DIM, (h + 1) * HEAD_DIM)
            add = carried[rows] * lead_ref[h : h + 1, at]
            out_ref[rows, at] = (y_ref[rows, at].astype(F32) + add).astype(BF16)


def last_kernel(chunks, late, late_group, x_ref, maps_ref, step_ref, sums_ref, skip_ref, enter_ref, y_ref, lead_ref,
                out_ref, state_scr):
    g = pl.program_id(0)
    is_late = (lax.rem(g, 2) == 0) & (g < 2 * late)

    @pl.when(is_late)
    def _():
        local_kernel(chunks, True, late_group, x_ref, maps_ref, step_ref, sums_ref, skip_ref, enter_ref, out_ref, state_scr)

    @pl.when(jnp.logical_not(is_late))
    def _():
        carried_group(chunks, y_ref, maps_ref, lead_ref, enter_ref, out_ref)


def local(raw_inputs, state_maps, step_size, log_decay, conv_weight, conv_bias, skip_gain, axis):
    channels, tokens = raw_inputs.shape
    heads = skip_gain.shape[0]
    groups = heads // GROUP
    chunks = tokens // CHUNK
    count = lax.axis_size(axis)

    tail = lax.ppermute(
        raw_inputs[:, tokens - 3 :], axis, [(i, i + 1) for i in range(count - 1)]
    )

    block = lambda g: (g, 0)
    whole = lambda g: (0, 0)
    big = pl.BlockSpec((ROWS, tokens), block)
    rows8 = pl.BlockSpec((GROUP, tokens), block)
    maps = pl.BlockSpec((2 * STATE, tokens), whole)
    cost = lambda us: pl.CostEstimate(
        flops=int(us * 5e8), bytes_accessed=int(us * 1e6), transcendentals=0
    )
    params = pltpu.CompilerParams(dimension_semantics=("arbitrary",))
    packed = pltpu.CompilerParams(
        dimension_semantics=("arbitrary",)
    )

    values, sums, lead, message = pl.pallas_call(
        functools.partial(values_kernel, chunks),
        grid=(groups,),
        in_specs=[
            big,
            pl.BlockSpec((ROWS, 3), block),
            maps,
            rows8,
            rows8,
            pl.BlockSpec((4, ROWS), lambda g: (0, g)),
            pl.BlockSpec((1, ROWS), lambda g: (0, g)),
        ],
        out_specs=[big, rows8, rows8, pl.BlockSpec((2 * GROUP, 24, 128), lambda g: (g, 0, 0))],
        out_shape=[
            jax.ShapeDtypeStruct((channels, tokens), BF16),
            jax.ShapeDtypeStruct((heads, tokens), F32),
            jax.ShapeDtypeStruct((heads, tokens), F32),
            jax.ShapeDtypeStruct((count, 24, 128), BF16),
        ],
        scratch_shapes=[
            pltpu.VMEM((GROUP, 8, tokens), F32),
            pltpu.VMEM((ROWS, tokens), BF16),
        ],
        compiler_params=params,
        cost_estimate=cost(20),
        name="values",
    )(raw_inputs, tail, state_maps, step_size, log_decay, conv_weight, conv_bias.reshape(1, channels))

    got = lax.all_to_all(message, axis, 0, 0, tiled=True)


    scalars = pl.BlockSpec(memory_space=pltpu.SMEM)

    def local_part(first, number, previous, enter=None):
        shift = lambda g: (g + first, 0)
        specs = [
            pl.BlockSpec((ROWS, tokens), shift),
            maps,
            pl.BlockSpec((GROUP, tokens), shift),
            pl.BlockSpec((GROUP, tokens), shift),
            scalars,
        ]
        arrays = [values, state_maps, step_size, sums, skip_gain]
        alias = {}
        if enter is not None:
            specs.append(pl.BlockSpec((2 * GROUP, 16, 128), lambda g: (g + first, 0, 0)))
            arrays.append(enter)
        if previous is not None:
            alias = {len(arrays): 0}
            specs.append(pl.BlockSpec(memory_space=pl.ANY))
            arrays.append(previous)
        return pl.pallas_call(
            functools.partial(local_kernel, chunks, enter is not None, lambda g: g + first),
            grid=(number,),
            in_specs=specs,
            out_specs=pl.BlockSpec((ROWS, tokens), shift),
            out_shape=jax.ShapeDtypeStruct((channels, tokens), BF16),
            scratch_shapes=[pltpu.VMEM((ROWS, STATE), F32)],
            input_output_aliases=alias,
            compiler_params=packed,
            cost_estimate=cost(8 * number),
            name="inside",
        )(*arrays)

    early, middle = EARLY, EARLY + MIDDLE
    partial = local_part(0, early, None)

    entering = pl.pallas_call(
        scan_kernel,
        in_specs=[pl.BlockSpec(memory_space=pltpu.VMEM)],
        out_specs=pl.BlockSpec(memory_space=pltpu.VMEM),
        out_shape=jax.ShapeDtypeStruct((count, 16, 128), BF16),
        cost_estimate=cost(3),
        name="scan",
    )(got)
    back = lax.all_to_all(entering, axis, 0, 0, tiled=True)

    partial = local_part(early, middle - early, partial)
    late = groups - middle

    def late_group(g):
        return middle + jnp.minimum((g + 1) // 2, late - 1)

    def early_group(g):
        return jnp.where(g >= 2 * late, g - late, jnp.maximum(g - 1, 0) // 2)

    def own_group(g):
        return jnp.where((g % 2 == 0) & (g < 2 * late), late_group(g), early_group(g))

    at_late = lambda g: (late_group(g), 0)
    at_early = lambda g: (early_group(g), 0)
    return pl.pallas_call(
        functools.partial(last_kernel, chunks, late, late_group),
        grid=(groups,),
        in_specs=[
            pl.BlockSpec((ROWS, tokens), at_late),
            maps,
            pl.BlockSpec((GROUP, tokens), at_late),
            pl.BlockSpec((GROUP, tokens), at_late),
            scalars,
            pl.BlockSpec((2 * GROUP, 16, 128), lambda g: (own_group(g), 0, 0)),
            pl.BlockSpec((ROWS, tokens), at_early),
            pl.BlockSpec((GROUP, tokens), at_early),
        ],
        out_specs=pl.BlockSpec((ROWS, tokens), lambda g: (own_group(g), 0)),
        out_shape=jax.ShapeDtypeStruct((channels, tokens), BF16),
        scratch_shapes=[pltpu.VMEM((ROWS, STATE), F32)],
        input_output_aliases={6: 0},
        compiler_params=packed,
        cost_estimate=cost(20),
        name="last",
    )(values, state_maps, step_size, sums, skip_gain, back, partial, lead)


def solution(mesh):
    axis = mesh.axis_names[0]
    return jax.shard_map(
        functools.partial(local, axis=axis),
        mesh=mesh,
        in_specs=(P(None, axis),) * 4 + (P(),) * 3,
        out_specs=P(None, axis),
        check_vma=False,
    )
```
